32 devices in a mesh: dp: 2 (over x), tp: 16 (over y, z, core).
Axes of the slice: x: 2, y: 2, z: 4, core: 2. Of those that a mesh axis runs over, the one named last changes fastest.
Arguments:
- x: bfloat16 [7168, 5120], P(('dp', 'tp')), parts along dimension 0
- dy: bfloat16 [7168, 5120], P(('dp', 'tp')), parts along dimension 0
- gate: bfloat16 [7168, 16384], P('dp', 'tp'), parts along dimension 0
- up: bfloat16 [7168, 16384], P('dp', 'tp'), parts along dimension 0
- w_gate: bfloat16 [5120, 16384], P(None, 'tp')
- w_up: bfloat16 [5120, 16384], P(None, 'tp')
- w_down: bfloat16 [16384, 5120], P('tp')
Outputs:
- output 1: bfloat16 [7168, 5120], P(('dp', 'tp')), parts along dimension 0
- output 2: bfloat16 [10240, 16384], P('dp', 'tp'), parts along dimension 0
- output 3: bfloat16 [10240, 16384], P('dp', 'tp'), parts along dimension 0
- output 4: bfloat16 [32768, 5120], P(('dp', 'tp')), parts along dimension 0
There are 2 independent parts. The reference program is written for one: setup_inputs(seed, part) draws one part's arguments, and reference() takes and returns one part's arrays. A program takes and returns all parts, laid end to end along the dimension named above; an argument that names none is the same for every part.
All inputs are finite; a program needn't handle non-finite values.
Results may differ from the reference program's by a relative error of at most 0.012.
Values are sent between devices in bfloat16 or wider.
A program may use at most 2 GiB of HBM per device.

```python
import jax
import jax.numpy as jnp

ROWS = 3584
D = 5120
FF = 16384


def act(gate, up):
    return jax.nn.silu(gate) * up


def setup_inputs(seed: int = 0, part: int = 0) -> dict:
    kx, ky, ka, kb, kg, ku, kd = jax.random.split(jax.random.key(seed), 7)
    kx, ky, ka, kb = (jax.random.fold_in(k, part) for k in (kx, ky, ka, kb))
    drawn = {
        "x": jax.random.normal(kx, (ROWS, D), jnp.float32),
        "dy": jax.random.normal(ky, (ROWS, D), jnp.float32),
        "gate": jax.random.normal(ka, (ROWS, FF), jnp.float32),
        "up": jax.random.normal(kb, (ROWS, FF), jnp.float32),
        "w_gate": jax.random.normal(kg, (D, FF), jnp.float32) * D**-0.5,
        "w_up": jax.random.normal(ku, (D, FF), jnp.float32) * D**-0.5,
        "w_down": jax.random.normal(kd, (FF, D), jnp.float32) * FF**-0.5,
    }
    return {k: v.astype(jnp.bfloat16) for k, v in drawn.items()}


def reference(x, dy, gate, up, w_gate, w_up, w_down):
    hidden, back = jax.vjp(act, gate.astype(jnp.float32), up.astype(jnp.float32))
    d_hidden = jnp.dot(dy, w_down.T, preferred_element_type=jnp.float32)
    d_gate, d_up = (g.astype(jnp.bfloat16) for g in back(d_hidden))
    dx = jnp.dot(d_gate, w_gate.T, preferred_element_type=jnp.float32) + jnp.dot(d_up, w_up.T, preferred_element_type=jnp.float32)
    dw_gate = jnp.dot(x.T, d_gate, preferred_element_type=jnp.float32)
    dw_up = jnp.dot(x.T, d_up, preferred_element_type=jnp.float32)
    dw_down = jnp.dot(hidden.astype(jnp.bfloat16).T, dy, preferred_element_type=jnp.float32)
    return tuple(g.astype(jnp.bfloat16) for g in (dx, dw_gate, dw_up, dw_down))
```

```python
import functools

import jax
import jax.numpy as jnp
from jax import lax
from jax.experimental import pallas as pl
from jax.experimental.pallas import tpu as pltpu
from jax.sharding import PartitionSpec as P

MESH = pl.DeviceIdType.MESH
BF16, F32 = jnp.bfloat16, jnp.float32
NC = 4
BLOCKS = 8
LAG = 2
KEEP = 3
Y_X, RS_Y = 16, 32
A_END, B_END, N_END, L_T, C_END = 20, 25, 29, 33, 36


def order(p, z):
    near = jnp.where(z < 2, z, 3 - z)
    q = jnp.where((near == 1) & (p < 2), 1 - p, p)
    return jnp.where(z < 2, q, 3 - q)


def kernel(
    dims,
    x, dy, gate, up, wg, wu, wd,
    dx, dwg, dwu, dwd, gx, gdy, own, sib, ins, yin, dgs, dus, hids,
    own_b, sib_b, in_b, out_b,
    z_send, z_recv, y_send, y_recv, sib_send, sib_recv, own_send,
    rs_send, rs_recv, ry_send, ry_recv, dxs_recv, load_sem,
):
    R, D, F, TF, TN, TM, TM2, TND, TK, TV = dims
    C, B, T = R // NC, 2 * R, 2 * R * BLOCKS
    dp, tp = lax.axis_index("dp"), lax.axis_index("tp")
    y, z, c = tp // 8, (tp // 2) % 4, tp % 2
    sent, kept = (dy, x), (gdy, gx)

    def dev(yy, zz, cc):
        return dict(device_id=(dp, yy * 8 + zz * 2 + cc), device_id_type=MESH)

    def rows(ref, start, n):
        return ref.at[pl.ds(pl.multiple_of(start, 8), n)]

    def place(yy, zz, cc):
        return ((yy * 4 + zz) * 2 + cc) * R

    def step_of(d):
        return (z, jnp.minimum(z + 1, 3)) if d == 0 else (3 - z, jnp.maximum(z - 1, 0))

    def z_at(d, pos):
        return pos if d == 0 else 3 - pos

    def gather_z(d, a, t):
        pos, nxt = step_of(d)
        base = a * NC * (pos + 1)

        def copy(t, own_rows=False):
            s = jnp.clip(t - base, 0, 11)
            p, j = s // NC, s % NC
            there = rows(kept[a], place(y, z_at(d, jnp.maximum(pos - p, 0)), c) + j * C, C)
            src = rows(sent[a], j * C, C) if own_rows else there
            return pltpu.make_async_remote_copy(
                src, there, z_send.at[d, a, t % 4], z_recv.at[d, a, s], **dev(y, nxt, c))

        def active(t):
            return (pos < 3) & (t >= base) & (t < base + NC * (pos + 1))

        @pl.when(active(t - KEEP))
        def _():
            copy(t - KEEP).wait_send()

        @pl.when(active(t) & (t < base + NC))
        def _():
            copy(t, True).start()

        @pl.when(active(t) & (t >= base + NC))
        def _():
            copy(t).start()

    def to_sibling(a, ref_rows, idx, sem):
        return pltpu.make_async_remote_copy(ref_rows, ref_rows, sem, sib_recv.at[a, idx], **dev(y, z, 1 - c))

    def arrive_z(d, a, t):
        pos, _ = step_of(d)
        base = a * NC * pos + LAG

        def chunk(t):
            r = jnp.clip(t - base, 0, 11)
            src_z = z_at(d, jnp.maximum(pos - 1 - r // NC, 0))
            return r, rows(kept[a], place(y, src_z, c) + (r % NC) * C, C), y * 4 + src_z

        def active(t):
            return (pos > 0) & (t >= base) & (t < base + NC * pos)

        @pl.when(active(t - KEEP))
        def _():
            _, ref, idx = chunk(t - KEEP)
            to_sibling(a, ref, idx, sib_send.at[d, a, (t - KEEP) % 4]).wait_send()

        @pl.when(active(t))
        def _():
            r, ref, idx = chunk(t)
            pltpu.make_async_remote_copy(
                ref, ref, z_send.at[d, a, 0], z_recv.at[d, a, r], **dev(y, z, 1 - c)).wait_recv()
            to_sibling(a, ref, idx, sib_send.at[d, a, t % 4]).start()

    def gather_y(a, t):
        base = a * Y_X

        def copy(t, own_rows=False):
            s = jnp.clip(t - base, 0, 15)
            there = rows(kept[a], place(y, order(s // NC, z), c) + (s % NC) * C, C)
            src = rows(sent[a], (s % NC) * C, C) if own_rows else there
            return pltpu.make_async_remote_copy(
                src, there, y_send.at[a, t % 4], y_recv.at[a, s], **dev(1 - y, z, c))

        def active(t):
            return (t >= base) & (t < base + 4 * NC)

        @pl.when(active(t - KEEP))
        def _():
            copy(t - KEEP).wait_send()

        @pl.when(active(t) & (t < base + NC))
        def _():
            copy(t, True).start()

        @pl.when(active(t) & (t >= base + NC))
        def _():
            copy(t).start()

    def arrive_y(a, t, drain_only=False):
        base = a * Y_X + LAG

        def chunk(t):
            r = jnp.clip(t - base, 0, 15)
            q = order(r // NC, z)
            return r, rows(kept[a], place(1 - y, q, c) + (r % NC) * C, C), (1 - y) * 4 + q

        def active(t):
            return (t >= base) & (t < base + 4 * NC)

        @pl.when(active(t - KEEP))
        def _():
            _, ref, idx = chunk(t - KEEP)
            to_sibling(a, ref, idx, sib_send.at[2, a, (t - KEEP) % 4]).wait_send()

        if drain_only:
            return

        @pl.when(active(t))
        def _():
            r, ref, idx = chunk(t)
            pltpu.make_async_remote_copy(
                ref, ref, y_send.at[a, 0], y_recv.at[a, r], **dev(1 - y, z, c)).wait_recv()
            to_sibling(a, ref, idx, sib_send.at[2, a, t % 4]).start()

    def own_to_sibling(a):
        return pltpu.make_async_remote_copy(
            sent[a], rows(kept[a], place(y, z, c), R), own_send.at[a], sib_recv.at[a, y * 4 + z], **dev(y, z, 1 - c))

    def wait_sibling(a, idx):
        ref = rows(kept[a], idx * B, R)
        pltpu.make_async_remote_copy(ref, ref, own_send.at[a], sib_recv.at[a, idx], **dev(y, z, 1 - c)).wait_recv()

    def wait_partial(idx):
        ref = rows(sib, idx * R, R)
        pltpu.make_async_remote_copy(ref, ref, own_send.at[0], dxs_recv.at[idx], **dev(y, z, 1 - c)).wait_recv()

    def own_load(b, idx, j):
        return pltpu.make_async_copy(rows(own, idx * R + j * C, C), own_b.at[b], load_sem.at[b, 0])

    def sib_load(b, idx, j):
        return pltpu.make_async_copy(rows(sib, idx * R + j * C, C), sib_b.at[b], load_sem.at[b, 1])

    def in_load(b, n, d, k, j):
        return pltpu.make_async_copy(rows(ins.at[d], k * R + j * C, C), in_b.at[b, n], load_sem.at[b, 2 + n])

    def wait_in(d, k, j):
        ref = rows(ins.at[d], k * R + j * C, C)
        pltpu.make_async_remote_copy(
            ref, ref, rs_send.at[d, 0], rs_recv.at[d, k * NC + j], **dev(y, z, 1 - c)).wait_recv()

    def add(b, slot, n):
        @pl.loop(0, D // TV)
        def _(i):
            cols = pl.ds(pl.multiple_of(i * TV, 128), TV)
            total = own_b[b, :, cols] + sib_b[b, :, cols].astype(F32)
            for m in range(n):
                total = total + in_b[b, m, :, cols].astype(F32)
            out_b[b, slot, :, cols] = total.astype(BF16)

    def sum_state(d, t):
        pos, nxt = step_of(d)
        base = jnp.where(pos == 0, 9, jnp.where(pos == 1, 11, 16))
        first = jnp.where(pos == 0, 0, 2)
        last = jnp.where(pos == 2, 4, 6)
        on = (pos < 3) & (t >= base + NC * first) & (t < base + NC * last)
        u = jnp.clip(t - base, 0, 23)
        k, j = u // NC, u % NC
        to_pos = jnp.where(k < 2, 1, jnp.where(k < 4, 3, 2))
        other = (k == 1) | (k == 3) | (k == 4)
        idx = jnp.where(other, 1 - y, y) * 4 + z_at(d, to_pos)
        return on, pos, nxt, k, j, idx

    def sum_send(d, t, nxt, k, j):
        return pltpu.make_async_remote_copy(
            out_b.at[d, t % 3], rows(ins.at[d], k * R + j * C, C), rs_send.at[d, t % 3],
            rs_recv.at[d, k * NC + j], **dev(y, nxt, c))

    def sum_loads(d, t):
        on, pos, _, k, j, idx = sum_state(d, t)

        @pl.when(on)
        def _():
            @pl.when(j == 0)
            def _():
                wait_partial(idx)

            own_load(d, idx, j).start()
            sib_load(d, idx, j).start()

            @pl.when(pos > 0)
            def _():
                wait_in(d, k, j)
                in_load(d, 0, d, k, j).start()

    def sum_drain(d, t):
        was, _, nxt, k, j, _ = sum_state(d, t - KEEP)

        @pl.when(was)
        def _():
            sum_send(d, t - KEEP, nxt, k, j).wait_send()

    def sum_add(d, t):
        sum_drain(d, t)
        on, pos, nxt, k, j, idx = sum_state(d, t)

        @pl.when(on)
        def _():
            own_load(d, idx, j).wait()
            sib_load(d, idx, j).wait()

            @pl.when(pos > 0)
            def _():
                in_load(d, 0, d, k, j).wait()
                add(d, t % 3, 1)

            @pl.when(pos == 0)
            def _():
                add(d, t % 3, 0)

            sum_send(d, t, nxt, k, j).start()

    def last_in(pos, other):
        if other:
            return jnp.where(pos == 1, 1, jnp.where(pos == 2, 4, 3))
        return jnp.where(pos == 1, 0, jnp.where(pos == 2, 5, 2))

    def end_loads(b, j, other, start):
        idx = jnp.where(other, 1 - y, y) * 4 + z
        if start:
            @pl.when(j == 0)
            def _():
                wait_partial(idx)

        copies = [own_load(b, idx, j), sib_load(b, idx, j)]
        for copy in copies:
            copy.start() if start else copy.wait()
        for d, there, slot in ((0, z > 0, 0), (1, z < 3, jnp.where(z > 0, 1, 0))):
            pos, _ = step_of(d)
            k = last_in(pos, other)

            @pl.when(there)
            def _(d=d, k=k, slot=slot):
                if start:
                    wait_in(d, k, j)
                    in_load(b, slot, d, k, j).start()
                else:
                    in_load(b, slot, d, k, j).wait()

    middle = (z > 0) & (z < 3)
    y_set = jnp.where(z < 2, 1, 0)

    def y_copy(t):
        j = jnp.clip(t - RS_Y, 0, NC - 1)
        return pltpu.make_async_remote_copy(
            out_b.at[y_set, t % 3], rows(yin, j * C, C), ry_send.at[t % 3], ry_recv.at[j], **dev(1 - y, z, c))

    def y_on(t):
        return (t >= RS_Y) & (t < RS_Y + NC)

    def y_drain(t):
        @pl.when(y_on(t - KEEP))
        def _():
            y_copy(t - KEEP).wait_send()

    def y_loads(t):
        @pl.when(y_on(t))
        def _():
            end_loads(y_set, t - RS_Y, True, True)

    def y_sum(t):
        y_drain(t)

        @pl.when(y_on(t))
        def _():
            end_loads(y_set, t - RS_Y, True, False)

            @pl.when(middle)
            def _():
                add(y_set, t % 3, 2)

            @pl.when(jnp.logical_not(middle))
            def _():
                add(y_set, t % 3, 1)

            y_copy(t).start()

    def clear(ref):
        high = min(64, ref.shape[0])

        @pl.loop(0, ref.shape[0] // high)
        def _(i):
            ref[pl.ds(pl.multiple_of(i * high, 8), high), :] = jnp.zeros((high, ref.shape[1]), F32)

    def exchange(t, late):
        for a in (0, 1):
            for d in (0, 1):
                arrive_z(d, a, t)
            arrive_y(a, t)
        for a in (0, 1):
            gather_y(a, t)
            for d in (0, 1):
                gather_z(d, a, t)
        for d in (0, 1):
            sum_loads(d, t)
        if late:
            y_loads(t)

    def sums(t, late):
        for d in (0, 1):
            sum_add(d, t)
        if late:
            y_sum(t)

    def spread(t, late, begin, end, step):
        @pl.loop(0, jnp.maximum(end - begin, 2))
        def _(n):
            @pl.when(n == 1)
            def _():
                sums(t, late)

            @pl.when(begin + n < end)
            def _():
                step(begin + n)

    barrier = pltpu.get_barrier_semaphore()
    pl.semaphore_signal(barrier, 1, **dev(y, z, 1 - c))
    pl.semaphore_signal(barrier, 1, **dev(1 - y, z, c))

    @pl.when(z < 3)
    def _():
        pl.semaphore_signal(barrier, 1, **dev(y, z + 1, c))

    @pl.when(z > 0)
    def _():
        pl.semaphore_signal(barrier, 1, **dev(y, z - 1, c))

    pl.semaphore_wait(barrier, jnp.where((z > 0) & (z < 3), 4, 3))
    for a in (0, 1):
        own_to_sibling(a).start()

    def first(wd_v, wg_v, wu_v, dy_v, gate_v, up_v, dg_v, du_v, hid_v, stf, stb, w_sem, b_sem, dy_sem, g_sem, st_sem, dx_sem, dxs_send):
        weights = [pltpu.make_async_copy(h, v, w_sem.at[i]) for i, (h, v) in enumerate(((wd, wd_v), (wg, wg_v), (wu, wu_v)))]

        def block_of(n):
            other = (n // 2) % 2
            return jnp.where(other == 1, 1 - y, y) * 4 + order(n % 2 + 2 * (n // 4), z)

        def gate_up(n):
            at = block_of(n) * B
            return [pltpu.make_async_copy(rows(h, at, B), v, g_sem.at[i]) for i, (h, v) in enumerate(((gate, gate_v), (up, up_v)))]

        def kept_grads(n):
            at = block_of(n) * B
            pairs = ((dg_v, dgs), (du_v, dus), (hid_v, hids))
            return [pltpu.make_async_copy(v, rows(h, at, B), st_sem.at[i]) for i, (v, h) in enumerate(pairs)]

        def own_rows(i, a):
            part = rows(dy_v, a * R, R)
            if i == 0:
                return pltpu.make_async_copy(sent[a], part, b_sem.at[a])
            return pltpu.make_async_copy(part, rows(kept[a], place(y, z, c), R), b_sem.at[a])

        def terms(n, tile, slot):
            at, cols = block_of(n) * R, pl.ds(pl.multiple_of(tile * TN, 128), TN)
            mine = pltpu.make_async_copy(
                stf.at[slot, pl.ds(pl.multiple_of(c * R, 8), R)], own.at[pl.ds(pl.multiple_of(at, 8), R), cols], dx_sem.at[slot])
            theirs = pltpu.make_async_remote_copy(
                stb.at[slot, pl.ds(pl.multiple_of((1 - c) * R, 8), R)], sib.at[pl.ds(pl.multiple_of(at, 8), R), cols],
                dxs_send.at[slot], dxs_recv.at[block_of(n)], **dev(y, z, 1 - c))
            return mine, theirs

        def wait_terms(n, tile, slot):
            mine, theirs = terms(n, tile, slot)
            mine.wait()
            theirs.wait_send()

        tiles = D // TN

        def drain(n):
            for copy in kept_grads(n):
                copy.wait()
            for slot in (0, 1):
                wait_terms(n, tiles - 2 + slot, slot)

        def gradients(n):
            @pl.when(n == 0)
            def _():
                weights[0].wait()

            for copy in gate_up(n):
                copy.wait()

            @pl.loop(0, F // TF)
            def _(i):
                cols = pl.ds(pl.multiple_of(i * TF, 128), TF)
                dh = lax.dot_general(
                    dy_v[...], wd_v[pl.ds(pl.multiple_of(i * TF, 128), TF), :], (((1,), (1,)), ((), ())), preferred_element_type=F32)
                g, u = gate_v[:, cols].astype(F32), up_v[:, cols].astype(F32)
                s = jax.nn.sigmoid(g)
                silu = g * s
                hid_v[:, cols] = (silu * u).astype(BF16)
                du_v[:, cols] = (dh * silu).astype(BF16)
                dg_v[:, cols] = ((dh * u) * (s * (1.0 + g * (1.0 - s)))).astype(BF16)

            for copy in kept_grads(n):
                copy.start()

            @pl.when(n < BLOCKS - 1)
            def _():
                for copy in gate_up(n + 1):
                    copy.start()

        def dx_terms(t, n):
            @pl.when(n == 0)
            def _():
                weights[1].wait()
                weights[2].wait()

            @pl.loop(0, tiles)
            def _(tile):
                @pl.when(tile == 1)
                def _():
                    sums(t, False)

                slot = tile % 2
                @pl.when(tile >= 2)
                def _():
                    wait_terms(n, tile - 2, slot)

                at = pl.ds(pl.multiple_of(tile * TN, 128), TN)
                nt = (((1,), (1,)), ((), ()))
                total = lax.dot_general(dg_v[...], wg_v[at, :], nt, preferred_element_type=F32)
                total = total + lax.dot_general(du_v[...], wu_v[at, :], nt, preferred_element_type=F32)
                stf[slot] = total
                stb[slot] = total.astype(BF16)
                mine, theirs = terms(n, tile, slot)
                mine.start()
                theirs.start()

        @pl.loop(0, A_END)
        def _(t):
            exchange(t, False)

            @pl.when(t == 0)
            def _():
                for a in (0, 1):
                    own_rows(0, a).start()
                for copy in gate_up(0) + weights:
                    copy.start()

            @pl.when(t == 1)
            def _():
                for a in (0, 1):
                    own_rows(0, a).wait()
                    own_rows(1, a).start()
                for a in (0, 1):
                    own_rows(1, a).wait()

            n = jnp.maximum((t - 4) // 2, 0)

            @pl.when((t == 2) | ((t >= 6) & (t % 2 == 0)))
            def _():
                idx = block_of(n)
                wait_sibling(0, idx)
                load = pltpu.make_async_copy(rows(gdy, idx * B, B), dy_v, dy_sem)
                load.start()

                @pl.when(n > 0)
                def _():
                    drain(n - 1)

                sums(t, False)
                load.wait()
                gradients(n)

            @pl.when((t == 3) | ((t >= 7) & (t % 2 == 1)))
            def _():
                dx_terms(t, n)

        drain(BLOCKS - 1)

    pl.run_scoped(
        first,
        pltpu.VMEM((F, D), BF16), pltpu.VMEM((D, F), BF16), pltpu.VMEM((D, F), BF16),
        pltpu.VMEM((B, D), BF16), pltpu.VMEM((B, F), BF16), pltpu.VMEM((B, F), BF16),
        pltpu.VMEM((B, F), BF16), pltpu.VMEM((B, F), BF16), pltpu.VMEM((B, F), BF16),
        pltpu.VMEM((2, B, TN), F32), pltpu.VMEM((2, B, TN), BF16),
        pltpu.SemaphoreType.DMA((3,)), pltpu.SemaphoreType.DMA((2,)), pltpu.SemaphoreType.DMA,
        pltpu.SemaphoreType.DMA((2,)), pltpu.SemaphoreType.DMA((3,)), pltpu.SemaphoreType.DMA((2,)), pltpu.SemaphoreType.DMA((2,)),
    )

    def second(hid_v, dy_v, acc, out_v, h_sem, dy_sem, o_sem):
        depth, wide = T // TK, D // TND
        steps = depth * wide
        per_tick = -(-steps // (B_END - A_END))

        def tile(i):
            nt, kc = i // depth, i % depth
            return pltpu.make_async_copy(
                gdy.at[pl.ds(pl.multiple_of(kc * TK, 8), TK), pl.ds(pl.multiple_of(nt * TND, 128), TND)],
                dy_v.at[i % 2], dy_sem.at[i % 2])

        def result(nt):
            return pltpu.make_async_copy(out_v, dwd.at[:, pl.ds(pl.multiple_of(nt * TND, 128), TND)], o_sem)

        hidden = pltpu.make_async_copy(hids, hid_v, h_sem)
        hidden.start()
        tile(0).start()

        def step(i):
            nt, kc = i // depth, i % depth
            tile(i).wait()

            @pl.when(i + 1 < steps)
            def _():
                tile(i + 1).start()

            @pl.when(kc == 0)
            def _():
                clear(acc)

            acc[...] += lax.dot_general(
                hid_v[pl.ds(pl.multiple_of(kc * TK, 8), TK), :], dy_v[i % 2], (((0,), (0,)), ((), ())), preferred_element_type=F32)

            @pl.when(kc == depth - 1)
            def _():
                @pl.when(nt > 0)
                def _():
                    result(nt - 1).wait()

                out_v[...] = acc[...].astype(BF16)
                result(nt).start()

        @pl.loop(A_END, B_END)
        def _(t):
            exchange(t, False)

            @pl.when(t == A_END)
            def _():
                hidden.wait()

            begin = (t - A_END) * per_tick
            spread(t, False, begin, jnp.minimum(begin + per_tick, steps), step)

        result(wide - 1).wait()

    pl.run_scoped(
        second,
        pltpu.VMEM((T, F), BF16), pltpu.VMEM((2, TK, TND), BF16), pltpu.VMEM((F, TND), F32), pltpu.VMEM((F, TND), BF16),
        pltpu.SemaphoreType.DMA, pltpu.SemaphoreType.DMA((2,)), pltpu.SemaphoreType.DMA,
    )

    def third(acc):
        def near(d_v, x_v, d_sem, x_sem):
            steps = D // TM2
            per_tick = -(-steps // (N_END - B_END))
            half = pl.ds(pl.multiple_of(y * 4 * B, 8), 4 * B)
            grads = [pltpu.make_async_copy(h.at[half], d_v.at[:, pl.ds(i * F, F)], d_sem.at[i]) for i, h in enumerate((dgs, dus))]

            def tile(i):
                return pltpu.make_async_copy(gx.at[half, pl.ds(pl.multiple_of(i * TM2, 128), TM2)], x_v.at[i % 2], x_sem.at[i % 2])

            def step(i):
                tile(i).wait()

                @pl.when(i + 1 < steps)
                def _():
                    tile(i + 1).start()

                acc[pl.ds(pl.multiple_of(i * TM2, 8), TM2), :] = lax.dot_general(
                    x_v[i % 2], d_v[...], (((0,), (0,)), ((), ())), preferred_element_type=F32)

            for copy in grads:
                copy.start()

            @pl.loop(B_END, N_END)
            def _(t):
                exchange(t, False)

                @pl.when(t == B_END)
                def _():
                    for q in range(4):
                        wait_sibling(1, y * 4 + q)
                    tile(0).start()
                    for copy in grads:
                        copy.wait()

                begin = (t - B_END) * per_tick
                spread(t, False, begin, jnp.minimum(begin + per_tick, steps), step)

        pl.run_scoped(
            near,
            pltpu.VMEM((4 * B, 2 * F), BF16), pltpu.VMEM((2, 4 * B, TM2), BF16),
            pltpu.SemaphoreType.DMA((2,)), pltpu.SemaphoreType.DMA((2,)),
        )

        def far(d_v, x_v, out_v, d_sem, x_sem, o_sem):
            wide = D // TM
            steps = wide * 4
            early = wide * 3
            per_tick = -(-early // (L_T - N_END))
            last_per_tick = -(-wide // 2)

            def block_of(m):
                return (1 - y) * 4 + order(m, z)

            def grads(m):
                at = block_of(m) * B
                return [
                    pltpu.make_async_copy(rows(h, at, B), d_v.at[m % 2, :, pl.ds(i * F, F)], d_sem.at[m % 2, i])
                    for i, h in enumerate((dgs, dus))
                ]

            def tile(i):
                return pltpu.make_async_copy(
                    gx.at[pl.ds(pl.multiple_of(block_of(i // wide) * B, 8), B), pl.ds(pl.multiple_of((i % wide) * TM, 128), TM)],
                    x_v.at[i % 2], x_sem.at[i % 2])

            def results(mt):
                at = pl.ds(pl.multiple_of(mt * TM, 8), TM)
                return [pltpu.make_async_copy(out_v.at[i], h.at[at], o_sem.at[i]) for i, h in enumerate((dwg, dwu))]

            def fetch(i):
                @pl.when(i % wide == 0)
                def _():
                    wait_sibling(1, block_of(i // wide))

                tile(i).start()

            def step(i):
                m, mt = i // wide, i % wide

                @pl.when(mt == 0)
                def _():
                    for copy in grads(m):
                        copy.wait()

                    @pl.when(m < 3)
                    def _():
                        for copy in grads(m + 1):
                            copy.start()

                tile(i).wait()

                @pl.when((i + 1 < steps) & (i + 1 != early))
                def _():
                    fetch(i + 1)

                at = pl.ds(pl.multiple_of(mt * TM, 8), TM)
                acc[at, :] += lax.dot_general(x_v[i % 2], d_v[m % 2], (((0,), (0,)), ((), ())), preferred_element_type=F32)

                @pl.when(m == 3)
                def _():
                    @pl.when(mt > 0)
                    def _():
                        for copy in results(mt - 1):
                            copy.wait()

                    for n in (0, 1):
                        out_v[n] = acc[at, pl.ds(n * F, F)].astype(BF16)
                    for copy in results(mt):
                        copy.start()

            for copy in grads(0):
                copy.start()

            @pl.loop(N_END, C_END)
            def _(t):
                exchange(t, True)

                @pl.when(t == N_END)
                def _():
                    fetch(0)

                @pl.when(t == L_T)
                def _():
                    fetch(early)

                def first_of(t):
                    return jnp.where(
                        t < L_T, jnp.minimum((t - N_END) * per_tick, early), jnp.minimum(early + (t - L_T) * last_per_tick, steps))

                spread(t, True, first_of(t), first_of(t + 1), step)

            for copy in results(wide - 1):
                copy.wait()

        pl.run_scoped(
            far,
            pltpu.VMEM((2, B, 2 * F), BF16), pltpu.VMEM((2, B, TM), BF16), pltpu.VMEM((2, TM, F), BF16),
            pltpu.SemaphoreType.DMA((2, 2)), pltpu.SemaphoreType.DMA((2,)), pltpu.SemaphoreType.DMA((2,)),
        )

    pl.run_scoped(third, pltpu.VMEM((D, 2 * F), F32))

    for t in range(C_END, C_END + KEEP):
        arrive_y(1, t, True)
        for d in (0, 1):
            sum_drain(d, t)
        y_drain(t)
    for a in (0, 1):
        own_to_sibling(a).wait_send()
    out = lambda j: pltpu.make_async_copy(out_b.at[j % 2, 0], rows(dx, j * C, C), load_sem.at[j % 2, 5])
    for j in (0, 1):
        end_loads(j % 2, j, False, True)
    for j in range(NC):
        b = j % 2
        end_loads(b, j, False, False)
        ref = rows(yin, j * C, C)
        pltpu.make_async_remote_copy(ref, ref, ry_send.at[0], ry_recv.at[j], **dev(1 - y, z, c)).wait_recv()
        last = pltpu.make_async_copy(ref, in_b.at[b, jnp.where(middle, 2, 1)], load_sem.at[b, 4])
        last.start()
        last.wait()
        if j >= 2:
            out(j - 2).wait()

        @pl.when(middle)
        def _(b=b):
            add(b, 0, 3)

        @pl.when(jnp.logical_not(middle))
        def _(b=b):
            add(b, 0, 2)

        out(j).start()
        if j + 2 < NC:
            end_loads(b, j + 2, False, True)
    for j in (NC - 2, NC - 1):
        out(j).wait()


def fused(dims, x, dy, gate, up, wg, wu, wd):
    R, D, F = dims[:3]
    C, T = R // NC, 2 * R * BLOCKS
    hbm = pl.BlockSpec(memory_space=pl.ANY)
    shape = jax.ShapeDtypeStruct
    outs = (
        shape((R, D), BF16), shape((D, F), BF16), shape((D, F), BF16), shape((F, D), BF16),
        shape((T, D), BF16), shape((T, D), BF16), shape((T // 2, D), F32), shape((T // 2, D), BF16),
        shape((2, 6 * R, D), BF16), shape((R, D), BF16),
        shape((T, F), BF16), shape((T, F), BF16), shape((T, F), BF16),
    )
    dma = pltpu.SemaphoreType.DMA
    results = pl.pallas_call(
        functools.partial(kernel, dims),
        out_shape=outs,
        in_specs=[hbm] * 7,
        out_specs=[hbm] * len(outs),
        scratch_shapes=[
            pltpu.VMEM((2, C, D), F32), pltpu.VMEM((2, C, D), BF16), pltpu.VMEM((2, 3, C, D), BF16), pltpu.VMEM((2, 3, C, D), BF16),
            dma((2, 2, 4)), dma((2, 2, 12)), dma((2, 4)), dma((2, 16)), dma((3, 2, 4)), dma((2, 8)), dma((2,)),
            dma((2, 3)), dma((2, 24)), dma((3,)), dma((NC,)), dma((BLOCKS,)), dma((2, 6)),
        ],
        compiler_params=pltpu.CompilerParams(collective_id=0, has_side_effects=True, vmem_limit_bytes=67043328),
        name="mlp_backward",
    )(x, dy, gate, up, wg, wu, wd)
    return handed_on(*results[:4])


def handed_on(*arrays):
    pieces = []
    for n, a in enumerate(arrays):
        count = next(k for k in (10, 8, 2) if a.shape[0] % (8 * k) == 0)
        pieces += [(n, i * (a.shape[0] // count), a.shape[0] // count) for i in range(count)]

    def kernel(*refs):
        ins, outs, held = refs[:4], refs[4:8], refs[8:12]
        sems = refs[12]

        def copy(way, i):
            n, at, high = pieces[i]
            part = pl.ds(at, high)
            src, dst = ((ins, held), (held, outs))[way]
            return pltpu.make_async_copy(src[n].at[part], dst[n].at[part], sems.at[way, i])

        for i in range(len(pieces)):
            copy(0, i).start()
        for i in range(len(pieces)):
            copy(0, i).wait()
            copy(1, i).start()
        for i in range(len(pieces)):
            copy(1, i).wait()

    hbm = pl.BlockSpec(memory_space=pl.ANY)
    return pl.pallas_call(
        kernel,
        out_shape=[jax.ShapeDtypeStruct(a.shape, a.dtype) for a in arrays],
        in_specs=[hbm] * 4,
        out_specs=[hbm] * 4,
        scratch_shapes=[pltpu.VMEM(a.shape, a.dtype) for a in arrays] + [pltpu.SemaphoreType.DMA((2, len(pieces)))],
        compiler_params=pltpu.CompilerParams(vmem_limit_bytes=67043328),
        name="hand_on",
    )(*arrays)


def solution(mesh):
    def step(x, dy, gate, up, wg, wu, wd):
        (rows, depth), wide = x.shape, wg.shape[1]
        dims = (rows, depth, wide, 512, 1024, 512, 256, 1280, 512, 1024)
        return fused(dims, x, dy, gate, up, wg, wu, wd)

    tokens, columns = P(("dp", "tp"), None), P("dp", "tp")
    return jax.shard_map(
        step,
        mesh=mesh,
        in_specs=(tokens, tokens, columns, columns, P(None, "tp"), P(None, "tp"), P("tp", None)),
        out_specs=(tokens, columns, columns, tokens),
        check_vma=False,
    )
```

```python
import functools

import jax
import jax.numpy as jnp
from jax import lax
from jax.experimental import pallas as pl
from jax.experimental.pallas import tpu as pltpu
from jax.sharding import PartitionSpec as P

MESH = pl.DeviceIdType.MESH
BF16, F32 = jnp.bfloat16, jnp.float32
NC = 4
BLOCKS = 8
LAG = 2
KEEP = 3
Y_X = 16
MINE, OTHERS = 26, 30
A_END, B_END, N_END, T_END = 20, 25, 29, 34


def order(p, z):
    near = jnp.where(z < 2, z, 3 - z)
    q = jnp.where((near == 1) & (p < 2), 1 - p, p)
    return jnp.where(z < 2, q, 3 - q)


def kernel(
    dims,
    x, dy, gate, up, wg, wu, wd,
    ysum, mysum, dwd, part, gx, gdy, own, sib, ins, dgs, dus, hids,
    own_b, sib_b, in_b, out_b,
    z_send, z_recv, y_send, y_recv, sib_send, sib_recv, own_send,
    rs_send, rs_recv, dxs_recv, load_sem, end_sem,
):
    R, D, F, TF, TN, TM, TND, TK, TV = dims
    C, B, T = R // NC, 2 * R, 2 * R * BLOCKS
    dp, tp = lax.axis_index("dp"), lax.axis_index("tp")
    y, z, c = tp // 8, (tp // 2) % 4, tp % 2
    sent, kept = (dy, x), (gdy, gx)

    def dev(yy, zz, cc):
        return dict(device_id=(dp, yy * 8 + zz * 2 + cc), device_id_type=MESH)

    def rows(ref, start, n):
        return ref.at[pl.ds(pl.multiple_of(start, 8), n)]

    def place(yy, zz, cc):
        return ((yy * 4 + zz) * 2 + cc) * R

    def step_of(d):
        return (z, jnp.minimum(z + 1, 3)) if d == 0 else (3 - z, jnp.maximum(z - 1, 0))

    def z_at(d, pos):
        return pos if d == 0 else 3 - pos

    def gather_z(d, a, t):
        pos, nxt = step_of(d)
        base = a * NC * (pos + 1)

        def copy(t, own_rows=False):
            s = jnp.clip(t - base, 0, 11)
            p, j = s // NC, s % NC
            there = rows(kept[a], place(y, z_at(d, jnp.maximum(pos - p, 0)), c) + j * C, C)
            src = rows(sent[a], j * C, C) if own_rows else there
            return pltpu.make_async_remote_copy(
                src, there, z_send.at[d, a, t % 4], z_recv.at[d, a, s], **dev(y, nxt, c))

        def active(t):
            return (pos < 3) & (t >= base) & (t < base + NC * (pos + 1))

        @pl.when(active(t - KEEP))
        def _():
            copy(t - KEEP).wait_send()

        @pl.when(active(t) & (t < base + NC))
        def _():
            copy(t, True).start()

        @pl.when(active(t) & (t >= base + NC))
        def _():
            copy(t).start()

    def to_sibling(a, ref_rows, idx, sem):
        return pltpu.make_async_remote_copy(ref_rows, ref_rows, sem, sib_recv.at[a, idx], **dev(y, z, 1 - c))

    def arrive_z(d, a, t):
        pos, _ = step_of(d)
        base = a * NC * pos + LAG

        def chunk(t):
            r = jnp.clip(t - base, 0, 11)
            src_z = z_at(d, jnp.maximum(pos - 1 - r // NC, 0))
            return r, rows(kept[a], place(y, src_z, c) + (r % NC) * C, C), y * 4 + src_z

        def active(t):
            return (pos > 0) & (t >= base) & (t < base + NC * pos)

        @pl.when(active(t - KEEP))
        def _():
            _, ref, idx = chunk(t - KEEP)
            to_sibling(a, ref, idx, sib_send.at[d, a, (t - KEEP) % 4]).wait_send()

        @pl.when(active(t))
        def _():
            r, ref, idx = chunk(t)
            pltpu.make_async_remote_copy(
                ref, ref, z_send.at[d, a, 0], z_recv.at[d, a, r], **dev(y, z, 1 - c)).wait_recv()
            to_sibling(a, ref, idx, sib_send.at[d, a, t % 4]).start()

    def gather_y(a, t):
        base = a * Y_X

        def copy(t, own_rows=False):
            s = jnp.clip(t - base, 0, 15)
            there = rows(kept[a], place(y, order(s // NC, z), c) + (s % NC) * C, C)
            src = rows(sent[a], (s % NC) * C, C) if own_rows else there
            return pltpu.make_async_remote_copy(
                src, there, y_send.at[a, t % 4], y_recv.at[a, s], **dev(1 - y, z, c))

        def active(t):
            return (t >= base) & (t < base + 4 * NC)

        @pl.when(active(t - KEEP))
        def _():
            copy(t - KEEP).wait_send()

        @pl.when(active(t) & (t < base + NC))
        def _():
            copy(t, True).start()

        @pl.when(active(t) & (t >= base + NC))
        def _():
            copy(t).start()

    def arrive_y(a, t):
        base = a * Y_X + LAG

        def chunk(t):
            r = jnp.clip(t - base, 0, 15)
            q = order(r // NC, z)
            return r, rows(kept[a], place(1 - y, q, c) + (r % NC) * C, C), (1 - y) * 4 + q

        def active(t):
            return (t >= base) & (t < base + 4 * NC)

        @pl.when(active(t - KEEP))
        def _():
            _, ref, idx = chunk(t - KEEP)
            to_sibling(a, ref, idx, sib_send.at[2, a, (t - KEEP) % 4]).wait_send()

        @pl.when(active(t))
        def _():
            r, ref, idx = chunk(t)
            pltpu.make_async_remote_copy(
                ref, ref, y_send.at[a, 0], y_recv.at[a, r], **dev(1 - y, z, c)).wait_recv()
            to_sibling(a, ref, idx, sib_send.at[2, a, t % 4]).start()

    def own_to_sibling(a):
        return pltpu.make_async_remote_copy(
            sent[a], rows(kept[a], place(y, z, c), R), own_send.at[a], sib_recv.at[a, y * 4 + z], **dev(y, z, 1 - c))

    def wait_sibling(a, idx):
        ref = rows(kept[a], idx * B, R)
        pltpu.make_async_remote_copy(ref, ref, own_send.at[a], sib_recv.at[a, idx], **dev(y, z, 1 - c)).wait_recv()

    def wait_partial(idx):
        ref = rows(sib, idx * R, R)
        pltpu.make_async_remote_copy(ref, ref, own_send.at[0], dxs_recv.at[idx], **dev(y, z, 1 - c)).wait_recv()

    def own_load(b, idx, j):
        return pltpu.make_async_copy(rows(own, idx * R + j * C, C), own_b.at[b], load_sem.at[b, 0])

    def sib_load(b, idx, j):
        return pltpu.make_async_copy(rows(sib, idx * R + j * C, C), sib_b.at[b], load_sem.at[b, 1])

    def in_load(b, n, d, k, j):
        return pltpu.make_async_copy(rows(ins.at[d], k * R + j * C, C), in_b.at[b, n], load_sem.at[b, 2 + n])

    def wait_in(d, k, j):
        ref = rows(ins.at[d], k * R + j * C, C)
        pltpu.make_async_remote_copy(
            ref, ref, rs_send.at[d, 0], rs_recv.at[d, k * NC + j], **dev(y, z, 1 - c)).wait_recv()

    def add(b, slot, n):
        @pl.loop(0, D // TV)
        def _(i):
            cols = pl.ds(pl.multiple_of(i * TV, 128), TV)
            total = own_b[b, :, cols] + sib_b[b, :, cols].astype(F32)
            for m in range(n):
                total = total + in_b[b, m, :, cols].astype(F32)
            if slot is None:
                own_b[b, :, cols] = total
            else:
                out_b[b, slot, :, cols] = total.astype(BF16)

    def sum_state(d, t):
        pos, nxt = step_of(d)
        on = (pos < 3) & (t >= 8 + 8 * pos) & (t < 32)
        u = jnp.clip(t - 8 - 4 * pos, 0, 23)
        k, j = u // NC, u % NC
        to_pos = jnp.where(k < 3, k + 1, 6 - k)
        idx = jnp.where(k < 3, y, 1 - y) * 4 + z_at(d, to_pos)
        return on, pos, nxt, k, j, idx

    def sum_send(d, t, nxt, k, j):
        return pltpu.make_async_remote_copy(
            out_b.at[d, t % 3], rows(ins.at[d], k * R + j * C, C), rs_send.at[d, t % 3],
            rs_recv.at[d, k * NC + j], **dev(y, nxt, c))

    def sum_loads(d, t):
        on, pos, _, k, j, idx = sum_state(d, t)

        @pl.when(on)
        def _():
            @pl.when(j == 0)
            def _():
                wait_partial(idx)

            own_load(d, idx, j).start()
            sib_load(d, idx, j).start()

            @pl.when(pos > 0)
            def _():
                wait_in(d, k, j)
                in_load(d, 0, d, k, j).start()

    def sum_drain(d, t):
        was, _, nxt, k, j, _ = sum_state(d, t - KEEP)

        @pl.when(was)
        def _():
            sum_send(d, t - KEEP, nxt, k, j).wait_send()

    def sum_add(d, t):
        sum_drain(d, t)
        on, pos, nxt, k, j, idx = sum_state(d, t)

        @pl.when(on)
        def _():
            own_load(d, idx, j).wait()
            sib_load(d, idx, j).wait()

            @pl.when(pos > 0)
            def _():
                in_load(d, 0, d, k, j).wait()
                add(d, t % 3, 1)

            @pl.when(pos == 0)
            def _():
                add(d, t % 3, 0)

            sum_send(d, t, nxt, k, j).start()

    end, middle = 2, (z > 0) & (z < 3)

    def end_loads(other, j, start):
        idx = jnp.where(other, 1 - y, y) * 4 + z
        if start:
            @pl.when(j == 0)
            def _():
                wait_partial(idx)

        for copy in (own_load(end, idx, j), sib_load(end, idx, j)):
            copy.start() if start else copy.wait()
        for d, there, slot in ((0, z > 0, 0), (1, z < 3, jnp.where(z > 0, 1, 0))):
            pos, _ = step_of(d)
            k = jnp.where(other, 6 - pos, pos - 1)

            @pl.when(there)
            def _(d=d, k=k, slot=slot):
                if start:
                    wait_in(d, k, j)
                    in_load(end, slot, d, k, j).start()
                else:
                    in_load(end, slot, d, k, j).wait()

    def end_state(t):
        other = t >= OTHERS
        return (t >= MINE) & (t < OTHERS + NC), other, jnp.clip(jnp.where(other, t - OTHERS, t - MINE), 0, NC - 1)

    def end_store(t, start):
        on, other, j = end_state(t)
        for mine in (True, False):
            @pl.when(on & (other != mine))
            def _(mine=mine):
                src, dst = (own_b.at[end], mysum) if mine else (out_b.at[end, 0], ysum)
                copy = pltpu.make_async_copy(src, rows(dst, j * C, C), end_sem)
                copy.start() if start else copy.wait()

    def last_loads(t):
        end_store(t - 1, False)
        on, other, j = end_state(t)

        @pl.when(on)
        def _():
            end_loads(other, j, True)

    def last_sum(t):
        on, other, j = end_state(t)

        @pl.when(on)
        def _():
            end_loads(other, j, False)

        for mine in (True, False):
            for n, where in ((2, middle), (1, jnp.logical_not(middle))):
                @pl.when(on & (other != mine) & where)
                def _(mine=mine, n=n):
                    add(end, None if mine else 0, n)

        end_store(t, True)

    def clear(ref):
        high = min(64, ref.shape[0])

        @pl.loop(0, ref.shape[0] // high)
        def _(i):
            ref[pl.ds(pl.multiple_of(i * high, 8), high), :] = jnp.zeros((high, ref.shape[1]), F32)

    def exchange(t, late):
        for a in (0, 1):
            for d in (0, 1):
                arrive_z(d, a, t)
            arrive_y(a, t)
        for a in (0, 1):
            gather_y(a, t)
            for d in (0, 1):
                gather_z(d, a, t)
        for d in (0, 1):
            sum_loads(d, t)
        if late:
            last_loads(t)

    def sums(t, late):
        for d in (0, 1):
            sum_add(d, t)
        if late:
            last_sum(t)

    def spread(t, late, begin, end, step):
        @pl.loop(0, jnp.maximum(end - begin, 2))
        def _(n):
            @pl.when(n == 1)
            def _():
                sums(t, late)

            @pl.when(begin + n < end)
            def _():
                step(begin + n)

    barrier = pltpu.get_barrier_semaphore()
    pl.semaphore_signal(barrier, 1, **dev(y, z, 1 - c))
    pl.semaphore_signal(barrier, 1, **dev(1 - y, z, c))

    @pl.when(z < 3)
    def _():
        pl.semaphore_signal(barrier, 1, **dev(y, z + 1, c))

    @pl.when(z > 0)
    def _():
        pl.semaphore_signal(barrier, 1, **dev(y, z - 1, c))

    pl.semaphore_wait(barrier, jnp.where((z > 0) & (z < 3), 4, 3))
    for a in (0, 1):
        own_to_sibling(a).start()

    def first(wd_v, wg_v, wu_v, dy_v, gate_v, up_v, dg_v, du_v, hid_v, stf, stb, w_sem, b_sem, dy_sem, g_sem, st_sem, dx_sem, dxs_send):
        weights = [pltpu.make_async_copy(h, v, w_sem.at[i]) for i, (h, v) in enumerate(((wd, wd_v), (wg, wg_v), (wu, wu_v)))]

        def block_of(n):
            other = (n == 2) | (n == 4) | (n >= 6)
            p = jnp.where(other, jnp.where(n == 7, 3, n // 2 - 1), jnp.where(n < 2, n, (n + 1) // 2))
            return jnp.where(other, 1 - y, y) * 4 + order(p, z)

        def gate_up(n):
            at = block_of(n) * B
            return [pltpu.make_async_copy(rows(h, at, B), v, g_sem.at[i]) for i, (h, v) in enumerate(((gate, gate_v), (up, up_v)))]

        def kept_grads(n):
            at = block_of(n) * B
            pairs = ((dg_v, dgs), (du_v, dus), (hid_v, hids))
            return [pltpu.make_async_copy(v, rows(h, at, B), st_sem.at[i]) for i, (v, h) in enumerate(pairs)]

        def own_rows(i, a):
            part = rows(dy_v, a * R, R)
            if i == 0:
                return pltpu.make_async_copy(sent[a], part, b_sem.at[a])
            return pltpu.make_async_copy(part, rows(kept[a], place(y, z, c), R), b_sem.at[a])

        def terms(n, tile, slot):
            at, cols = block_of(n) * R, pl.ds(pl.multiple_of(tile * TN, 128), TN)
            mine = pltpu.make_async_copy(
                stf.at[slot, pl.ds(pl.multiple_of(c * R, 8), R)], own.at[pl.ds(pl.multiple_of(at, 8), R), cols], dx_sem.at[slot])
            theirs = pltpu.make_async_remote_copy(
                stb.at[slot, pl.ds(pl.multiple_of((1 - c) * R, 8), R)], sib.at[pl.ds(pl.multiple_of(at, 8), R), cols],
                dxs_send.at[slot], dxs_recv.at[block_of(n)], **dev(y, z, 1 - c))
            return mine, theirs

        def wait_terms(n, tile, slot):
            mine, theirs = terms(n, tile, slot)
            mine.wait()
            theirs.wait_send()

        tiles = D // TN

        def drain(n):
            for copy in kept_grads(n):
                copy.wait()
            for tile in (tiles - 2, tiles - 1):
                wait_terms(n, tile, tile % 2)

        def gradients(n):
            @pl.when(n == 0)
            def _():
                weights[0].wait()

            for copy in gate_up(n):
                copy.wait()

            @pl.loop(0, F // TF)
            def _(i):
                cols = pl.ds(pl.multiple_of(i * TF, 128), TF)
                dh = lax.dot_general(
                    dy_v[...], wd_v[pl.ds(pl.multiple_of(i * TF, 128), TF), :], (((1,), (1,)), ((), ())), preferred_element_type=F32)
                g, u = gate_v[:, cols].astype(F32), up_v[:, cols].astype(F32)
                s = jax.nn.sigmoid(g)
                silu = g * s
                hid_v[:, cols] = (silu * u).astype(BF16)
                du_v[:, cols] = (dh * silu).astype(BF16)
                dg_v[:, cols] = ((dh * u) * (s * (1.0 + g * (1.0 - s)))).astype(BF16)

            for copy in kept_grads(n):
                copy.start()

            @pl.when(n < BLOCKS - 1)
            def _():
                for copy in gate_up(n + 1):
                    copy.start()

        def dx_terms(t, n):
            @pl.when(n == 0)
            def _():
                weights[1].wait()
                weights[2].wait()

            @pl.loop(0, tiles)
            def _(tile):
                @pl.when(tile == 1)
                def _():
                    sums(t, False)

                slot = tile % 2
                @pl.when(tile >= 2)
                def _():
                    wait_terms(n, tile - 2, slot)

                at = pl.ds(pl.multiple_of(tile * TN, 128), TN)
                nt = (((1,), (1,)), ((), ()))
                total = lax.dot_general(dg_v[...], wg_v[at, :], nt, preferred_element_type=F32)
                total = total + lax.dot_general(du_v[...], wu_v[at, :], nt, preferred_element_type=F32)
                stf[slot] = total
                stb[slot] = total.astype(BF16)
                mine, theirs = terms(n, tile, slot)
                mine.start()
                theirs.start()

            drain(n)

        @pl.loop(0, A_END)
        def _(t):
            exchange(t, False)

            @pl.when(t == 0)
            def _():
                for a in (0, 1):
                    own_rows(0, a).start()
                for copy in gate_up(0) + weights:
                    copy.start()

            @pl.when(t == 1)
            def _():
                for a in (0, 1):
                    own_rows(0, a).wait()
                    own_rows(1, a).start()
                for a in (0, 1):
                    own_rows(1, a).wait()

            n = jnp.maximum((t - 4) // 2, 0)

            @pl.when((t == 2) | ((t >= 6) & (t % 2 == 0)))
            def _():
                idx = block_of(n)
                wait_sibling(0, idx)
                load = pltpu.make_async_copy(rows(gdy, idx * B, B), dy_v, dy_sem)
                load.start()

                sums(t, False)
                load.wait()
                gradients(n)

            @pl.when((t == 3) | ((t >= 7) & (t % 2 == 1)))
            def _():
                dx_terms(t, n)

    pl.run_scoped(
        first,
        pltpu.VMEM((F, D), BF16), pltpu.VMEM((D, F), BF16), pltpu.VMEM((D, F), BF16),
        pltpu.VMEM((B, D), BF16), pltpu.VMEM((B, F), BF16), pltpu.VMEM((B, F), BF16),
        pltpu.VMEM((B, F), BF16), pltpu.VMEM((B, F), BF16), pltpu.VMEM((B, F), BF16),
        pltpu.VMEM((2, B, TN), F32), pltpu.VMEM((2, B, TN), BF16),
        pltpu.SemaphoreType.DMA((3,)), pltpu.SemaphoreType.DMA((2,)), pltpu.SemaphoreType.DMA,
        pltpu.SemaphoreType.DMA((2,)), pltpu.SemaphoreType.DMA((3,)), pltpu.SemaphoreType.DMA((2,)), pltpu.SemaphoreType.DMA((2,)),
    )

    def second(hid_v, dy_v, acc, out_v, h_sem, dy_sem, o_sem):
        depth, wide = T // TK, D // TND
        steps = depth * wide
        per_tick = -(-steps // (B_END - A_END))

        def tile(i):
            nt, kc = i // depth, i % depth
            return pltpu.make_async_copy(
                gdy.at[pl.ds(pl.multiple_of(kc * TK, 8), TK), pl.ds(pl.multiple_of(nt * TND, 128), TND)],
                dy_v.at[i % 2], dy_sem.at[i % 2])

        def result(nt):
            return pltpu.make_async_copy(out_v, dwd.at[:, pl.ds(pl.multiple_of(nt * TND, 128), TND)], o_sem)

        hidden = pltpu.make_async_copy(hids, hid_v, h_sem)
        hidden.start()
        tile(0).start()

        def step(i):
            nt, kc = i // depth, i % depth
            tile(i).wait()

            @pl.when(i + 1 < steps)
            def _():
                tile(i + 1).start()

            @pl.when(kc == 0)
            def _():
                clear(acc)

            acc[...] += lax.dot_general(
                hid_v[pl.ds(pl.multiple_of(kc * TK, 8), TK), :], dy_v[i % 2], (((0,), (0,)), ((), ())), preferred_element_type=F32)

            @pl.when(kc == depth - 1)
            def _():
                @pl.when(nt > 0)
                def _():
                    result(nt - 1).wait()

                out_v[...] = acc[...].astype(BF16)
                result(nt).start()

        @pl.loop(A_END, B_END)
        def _(t):
            exchange(t, False)

            @pl.when(t == A_END)
            def _():
                hidden.wait()

            begin = (t - A_END) * per_tick
            spread(t, False, begin, jnp.minimum(begin + per_tick, steps), step)

        result(wide - 1).wait()

    pl.run_scoped(
        second,
        pltpu.VMEM((T, F), BF16), pltpu.VMEM((2, TK, TND), BF16), pltpu.VMEM((F, TND), F32), pltpu.VMEM((F, TND), BF16),
        pltpu.SemaphoreType.DMA, pltpu.SemaphoreType.DMA((2,)), pltpu.SemaphoreType.DMA,
    )

    def third(d_v, x_v, out_v, d_sem, x_sem, o_sem):
        steps = D // TM
        per_tick = -(-steps // (N_END - B_END))
        half = pl.ds(pl.multiple_of(y * 4 * B, 8), 4 * B)
        grads = [pltpu.make_async_copy(h.at[half], d_v.at[:, pl.ds(i * F, F)], d_sem.at[i]) for i, h in enumerate((dgs, dus))]

        def tile(i):
            return pltpu.make_async_copy(gx.at[half, pl.ds(pl.multiple_of(i * TM, 128), TM)], x_v.at[i % 2], x_sem.at[i % 2])

        def result(i):
            return pltpu.make_async_copy(out_v.at[i % 2], part.at[pl.ds(pl.multiple_of(i * TM, 8), TM)], o_sem.at[i % 2])

        def step(i):
            tile(i).wait()

            @pl.when(i + 1 < steps)
            def _():
                tile(i + 1).start()

            @pl.when(i >= 2)
            def _():
                result(i - 2).wait()

            out_v[i % 2] = lax.dot_general(x_v[i % 2], d_v[...], (((0,), (0,)), ((), ())), preferred_element_type=F32)
            result(i).start()

        for copy in grads:
            copy.start()

        @pl.loop(B_END, N_END)
        def _(t):
            exchange(t, True)

            @pl.when(t == B_END)
            def _():
                for q in range(4):
                    wait_sibling(1, y * 4 + q)
                tile(0).start()
                for copy in grads:
                    copy.wait()

            begin = (t - B_END) * per_tick
            spread(t, True, begin, jnp.minimum(begin + per_tick, steps), step)

        for i in (steps - 2, steps - 1):
            result(i).wait()

    pl.run_scoped(
        third,
        pltpu.VMEM((4 * B, 2 * F), BF16), pltpu.VMEM((2, 4 * B, TM), BF16), pltpu.VMEM((2, TM, 2 * F), F32),
        pltpu.SemaphoreType.DMA((2,)), pltpu.SemaphoreType.DMA((2,)), pltpu.SemaphoreType.DMA((2,)),
    )

    @pl.loop(N_END, T_END + KEEP)
    def _(t):
        exchange(t, True)
        sums(t, True)

    for q in range(4):
        wait_sibling(1, (1 - y) * 4 + q)
    for a in (0, 1):
        own_to_sibling(a).wait_send()


def finish_kernel(dims, part, gx, dgs, dus, down, dwg, dwu, dwd, d_v, x_v, p_v, out_v, down_v, d_sem, x_sem, p_sem, o_sem, c_sem):
    R, D, F, TM = dims[0], dims[1], dims[2], dims[5]
    steps, depth = D // TM, gx.shape[0] // 2
    half = pl.ds(pl.multiple_of((1 - lax.axis_index("tp") // 8) * depth, 8), depth)
    grads = [pltpu.make_async_copy(h.at[half], d_v.at[:, pl.ds(i * F, F)], d_sem.at[i]) for i, h in enumerate((dgs, dus))]
    pieces, high = 8, F // 8

    def tiles(i):
        at = pl.multiple_of(i * TM, 128)
        return [
            pltpu.make_async_copy(gx.at[half, pl.ds(at, TM)], x_v.at[i % 2], x_sem.at[i % 2]),
            pltpu.make_async_copy(part.at[pl.ds(at, TM)], p_v.at[i % 2], p_sem.at[i % 2]),
        ]

    def results(i):
        at = pl.ds(pl.multiple_of(i * TM, 8), TM)
        return [pltpu.make_async_copy(out_v.at[i % 2, n], h.at[at], o_sem.at[i % 2, n]) for n, h in enumerate((dwg, dwu))]

    def piece(way, i):
        at = pl.ds(pl.multiple_of(i * high, 8), high)
        if way == 0:
            return pltpu.make_async_copy(down.at[at], down_v.at[at], c_sem.at[0, i])
        return pltpu.make_async_copy(down_v.at[at], dwd.at[at], c_sem.at[1, i])

    for copy in grads + tiles(0):
        copy.start()
    for copy in grads:
        copy.wait()
    for i in range(pieces):
        piece(0, i).start()

    @pl.loop(0, steps)
    def _(i):
        for copy in tiles(i):
            copy.wait()

        @pl.when(i + 1 < steps)
        def _():
            for copy in tiles(i + 1):
                copy.start()

        @pl.when(i < pieces)
        def _():
            piece(0, i).wait()
            piece(1, i).start()

        @pl.when(i >= 2)
        def _():
            for copy in results(i - 2):
                copy.wait()

        p_v[i % 2] += lax.dot_general(x_v[i % 2], d_v[...], (((0,), (0,)), ((), ())), preferred_element_type=F32)
        for n in (0, 1):
            out_v[i % 2, n] = p_v[i % 2, :, pl.ds(n * F, F)].astype(BF16)
        for copy in results(i):
            copy.start()

    for i in (steps - 2, steps - 1):
        for copy in results(i):
            copy.wait()
    for i in range(pieces):
        piece(1, i).wait()


def fused(dims, x, dy, gate, up, wg, wu, wd):
    R, D, F, TM = dims[0], dims[1], dims[2], dims[5]
    C, T = R // NC, 2 * R * BLOCKS
    hbm = pl.BlockSpec(memory_space=pl.ANY)
    shape, vmem, dma = jax.ShapeDtypeStruct, pltpu.VMEM, pltpu.SemaphoreType.DMA
    outs = (
        shape((R, D), BF16), shape((R, D), F32), shape((F, D), BF16), shape((D, 2 * F), F32),
        shape((T, D), BF16), shape((T, D), BF16), shape((T // 2, D), F32), shape((T // 2, D), BF16),
        shape((2, 6 * R, D), BF16), shape((T, F), BF16), shape((T, F), BF16), shape((T, F), BF16),
    )
    product = 2 * T * D * F
    ysum, mysum, down, part, gx, _, _, _, _, dgs, dus, _ = pl.pallas_call(
        functools.partial(kernel, dims),
        out_shape=outs,
        in_specs=[hbm] * 7,
        out_specs=[hbm] * len(outs),
        scratch_shapes=[
            vmem((3, C, D), F32), vmem((3, C, D), BF16), vmem((3, 2, C, D), BF16), vmem((3, 3, C, D), BF16),
            dma((2, 2, 4)), dma((2, 2, 12)), dma((2, 4)), dma((2, 16)), dma((3, 2, 4)), dma((2, 8)), dma((2,)),
            dma((2, 3)), dma((2, 24)), dma((BLOCKS,)), dma((3, 4)), dma,
        ],
        compiler_params=pltpu.CompilerParams(collective_id=0, has_side_effects=True, vmem_limit_bytes=67043328),
        cost_estimate=pl.CostEstimate(flops=5 * product, bytes_accessed=10 * T * D, transcendentals=0),
        name="mlp_backward",
    )(x, dy, gate, up, wg, wu, wd)
    across = lax.ppermute(ysum, "tp", [(i, (i + 8) % 16) for i in range(16)])
    weights = pl.pallas_call(
        functools.partial(finish_kernel, dims),
        out_shape=(shape((D, F), BF16), shape((D, F), BF16), shape((F, D), BF16)),
        in_specs=[hbm] * 5,
        out_specs=[hbm] * 3,
        scratch_shapes=[
            vmem((T // 2, 2 * F), BF16), vmem((2, T // 2, TM), BF16), vmem((2, TM, 2 * F), F32), vmem((2, 2, TM, F), BF16),
            vmem((F, D), BF16), dma((2,)), dma((2,)), dma((2,)), dma((2, 2)), dma((2, 8)),
        ],
        compiler_params=pltpu.CompilerParams(vmem_limit_bytes=67043328),
        cost_estimate=pl.CostEstimate(flops=product, bytes_accessed=6 * T * D, transcendentals=0),
        name="finish",
    )(part, gx, dgs, dus, down)
    return ((mysum + across.astype(F32)).astype(BF16), *weights)


def solution(mesh):
    def step(x, dy, gate, up, wg, wu, wd):
        (rows, depth), wide = x.shape, wg.shape[1]
        dims = (rows, depth, wide, 512, 1024, 256, 1280, 512, 1024)
        return fused(dims, x, dy, gate, up, wg, wu, wd)

    tokens, columns = P(("dp", "tp"), None), P("dp", "tp")
    return jax.shard_map(
        step,
        mesh=mesh,
        in_specs=(tokens, tokens, columns, columns, P(None, "tp"), P(None, "tp"), P("tp", None)),
        out_specs=(tokens, columns, columns, tokens),
        check_vma=False,
    )
```

```python
import functools

import jax
import jax.numpy as jnp
from jax import lax
from jax.experimental import pallas as pl
from jax.experimental.pallas import tpu as pltpu
from jax.sharding import PartitionSpec as P

MESH = pl.DeviceIdType.MESH
BF16, F32 = jnp.bfloat16, jnp.float32
NC = 4
BLOCKS = 8
LAG = 2
KEEP = 3
LATE = 3
Y_X, Y_X3 = 16, 20
CUT = 21
SUMS = 11
PARTS, OTHERS = 16, 28
A_END, B_END, N_END, T_END = 19, 25, 29, 33


def order(p, z):
    near = jnp.where(z < 2, z, 3 - z)
    q = jnp.where((near == 1) & (p < 2), 1 - p, p)
    return jnp.where(z < 2, q, 3 - q)


def kernel(
    dims,
    x, dy, gate, up, wg, wu, wd,
    ysum, mysum, next_sum, back_sum, dwd, part, gx, gdy, own, sib, ins, dgs, dus, hids,
    own_b, sib_b, in_b, out_b,
    z_send, z_recv, y_send, y_recv, short_send, sib_send, sib_recv, sib_short, own_send, cut_send, cut_recv, cut_sib,
    rs_send, rs_recv, dxs_recv, load_sem, end_sem,
):
    R, D, F, TF, TN, TM, TND, TK, TV, CUT_ROWS = dims
    C, B, T = R // NC, 2 * R, 2 * R * BLOCKS
    dp, tp = lax.axis_index("dp"), lax.axis_index("tp")
    y, z, c = tp // 8, (tp // 2) % 4, tp % 2
    sent, kept = (dy, x), (gdy, gx)

    def dev(yy, zz, cc):
        return dict(device_id=(dp, yy * 8 + zz * 2 + cc), device_id_type=MESH)

    def rows(ref, start, n):
        return ref.at[pl.ds(pl.multiple_of(start, 8), n)]

    def place(yy, zz, cc):
        return ((yy * 4 + zz) * 2 + cc) * R

    def step_of(d):
        return (z, jnp.minimum(z + 1, 3)) if d == 0 else (3 - z, jnp.maximum(z - 1, 0))

    def z_at(d, pos):
        return pos if d == 0 else 3 - pos

    def gather_z(d, a, t):
        pos, nxt = step_of(d)
        base = a * NC * (pos + 1)

        def copy(t, own_rows=False):
            s = jnp.clip(t - base, 0, 11)
            p, j = s // NC, s % NC
            there = rows(kept[a], place(y, z_at(d, jnp.maximum(pos - p, 0)), c) + j * C, C)
            src = rows(sent[a], j * C, C) if own_rows else there
            return pltpu.make_async_remote_copy(
                src, there, z_send.at[d, a, t % 4], z_recv.at[d, a, s], **dev(y, nxt, c))

        def active(t):
            return (pos < 3) & (t >= base) & (t < base + NC * (pos + 1))

        @pl.when(active(t - KEEP))
        def _():
            copy(t - KEEP).wait_send()

        @pl.when(active(t) & (t < base + NC))
        def _():
            copy(t, True).start()

        @pl.when(active(t) & (t >= base + NC))
        def _():
            copy(t).start()

    def to_sibling(a, ref_rows, idx, sem):
        return pltpu.make_async_remote_copy(ref_rows, ref_rows, sem, sib_recv.at[a, idx], **dev(y, z, 1 - c))

    def arrive_z(d, a, t):
        pos, _ = step_of(d)
        base = a * NC * pos + LAG

        def chunk(t):
            r = jnp.clip(t - base, 0, 11)
            src_z = z_at(d, jnp.maximum(pos - 1 - r // NC, 0))
            return r, rows(kept[a], place(y, src_z, c) + (r % NC) * C, C), y * 4 + src_z

        def active(t):
            return (pos > 0) & (t >= base) & (t < base + NC * pos)

        @pl.when(active(t - KEEP))
        def _():
            _, ref, idx = chunk(t - KEEP)
            to_sibling(a, ref, idx, sib_send.at[d, a, (t - KEEP) % 4]).wait_send()

        @pl.when(active(t))
        def _():
            r, ref, idx = chunk(t)
            pltpu.make_async_remote_copy(
                ref, ref, z_send.at[d, a, 0], z_recv.at[d, a, r], **dev(y, z, 1 - c)).wait_recv()
            to_sibling(a, ref, idx, sib_send.at[d, a, t % 4]).start()

    def y_chunk(a, t, short):
        if a == 0:
            s = jnp.clip(t, 0, 4 * NC - 1)
            return (t >= 0) & (t < 4 * NC), s // NC, s % NC, C
        v = jnp.clip(t - Y_X3, 0, 9)
        if short:
            return (t > Y_X3) & (t <= Y_X3 + 9) & (v % 3 == 0), jnp.maximum(v // 3, 1), 3, C - CUT_ROWS
        near = t < Y_X3
        return (t >= Y_X) & (t < Y_X3 + 9), jnp.where(near, 0, 1 + v // 3), jnp.where(near, jnp.clip(t - Y_X, 0, 3), v % 3), C

    def y_sems(a, t, short):
        return (short_send.at[(t // 3) % 2], sib_short.at[(t // 3) % 2]) if short else (y_send.at[a, t % 4], sib_send.at[2, a, t % 4])

    def gather_y(a, t, short=False):
        def copy(t, own_rows=False):
            _, p, j, high = y_chunk(a, t, short)
            there = rows(kept[a], place(y, order(p, z), c) + j * C, high)
            src = rows(sent[a], j * C, high) if own_rows else there
            return pltpu.make_async_remote_copy(src, there, y_sems(a, t, short)[0], y_recv.at[a, p * NC + j], **dev(1 - y, z, c))

        was, (on, p, _, _) = y_chunk(a, t - KEEP, short)[0], y_chunk(a, t, short)

        @pl.when(was)
        def _():
            copy(t - KEEP).wait_send()

        if not short:
            @pl.when(on & (p == 0))
            def _():
                copy(t, True).start()

        @pl.when(on & (p > 0))
        def _():
            copy(t).start()

    def arrive_y(a, t, short=False):
        def sent_at(t):
            if a == 0:
                return t - LAG
            return jnp.where(t < Y_X3 + LAG, t - LAG, jnp.where(t < Y_X3 + LATE, -1, t - LATE))

        def chunk(t):
            _, p, j, high = y_chunk(a, sent_at(t), short)
            q = order(p, z)
            return p * NC + j, rows(kept[a], place(1 - y, q, c) + j * C, high), (1 - y) * 4 + q

        @pl.when(y_chunk(a, sent_at(t - KEEP), short)[0])
        def _():
            _, ref, idx = chunk(t - KEEP)
            to_sibling(a, ref, idx, y_sems(a, t - KEEP, short)[1]).wait_send()

        @pl.when(y_chunk(a, sent_at(t), short)[0])
        def _():
            r, ref, idx = chunk(t)
            pltpu.make_async_remote_copy(ref, ref, y_send.at[a, 0], y_recv.at[a, r], **dev(1 - y, z, c)).wait_recv()
            to_sibling(a, ref, idx, y_sems(a, t, short)[1]).start()

    def pass_cut(d, t, arrive):
        pos, nxt = step_of(d)
        far = 1 if arrive else 0

        def state(t):
            ticks, last = ((CUT + 3, CUT + 6), (CUT + 6, CUT + 8, CUT + 10)) if arrive else ((CUT, CUT + 3), (CUT + 3, CUT + 4, CUT + 7))
            at_last = pos == 2 + far
            h = jnp.where(at_last, jnp.where(t == last[1], 1, jnp.where(t == last[2], 2, 0)), jnp.where(t == ticks[1], 1, 0))
            on = jnp.where(at_last, (t == last[0]) | (t == last[1]) | (t == last[2]), (t == ticks[0]) | (t == ticks[1]))
            on = on & (h + far <= pos) & (pos < 3 + far)
            q = z_at(d, jnp.maximum(pos - far - h, 0))
            ref = rows(gx, place(1 - y, q, c) + (R - CUT_ROWS), CUT_ROWS)
            if arrive:
                copy = to_sibling(1, ref, (1 - y) * 4 + q, cut_sib.at[d, h])
            else:
                copy = pltpu.make_async_remote_copy(ref, ref, cut_send.at[d, h], cut_recv.at[d, h], **dev(y, nxt, c))
            return on, h, ref, copy

        was, now = state(t - KEEP), state(t)

        @pl.when(was[0])
        def _():
            was[3].wait_send()

        @pl.when(now[0])
        def _():
            _, h, ref, copy = now
            if arrive:
                pltpu.make_async_remote_copy(ref, ref, cut_send.at[d, 0], cut_recv.at[d, h], **dev(y, z, 1 - c)).wait_recv()
            copy.start()

    def own_to_sibling(a):
        return pltpu.make_async_remote_copy(
            sent[a], rows(kept[a], place(y, z, c), R), own_send.at[a], sib_recv.at[a, y * 4 + z], **dev(y, z, 1 - c))

    def wait_sibling(a, idx):
        ref = rows(kept[a], idx * B, R)
        pltpu.make_async_remote_copy(ref, ref, own_send.at[a], sib_recv.at[a, idx], **dev(y, z, 1 - c)).wait_recv()

    def wait_partial(idx):
        ref = rows(sib, idx * R, R)
        pltpu.make_async_remote_copy(ref, ref, own_send.at[0], dxs_recv.at[idx], **dev(y, z, 1 - c)).wait_recv()

    def own_load(b, idx, j):
        return pltpu.make_async_copy(rows(own, idx * R + j * C, C), own_b.at[b], load_sem.at[b, 0])

    def sib_load(b, idx, j):
        return pltpu.make_async_copy(rows(sib, idx * R + j * C, C), sib_b.at[b], load_sem.at[b, 1])

    def in_load(b, n, d, k, j):
        return pltpu.make_async_copy(rows(ins.at[d], k * R + j * C, C), in_b.at[b, n], load_sem.at[b, 2 + n])

    def wait_in(d, k, j):
        ref = rows(ins.at[d], k * R + j * C, C)
        pltpu.make_async_remote_copy(
            ref, ref, rs_send.at[d, 0], rs_recv.at[d, k * NC + j], **dev(y, z, 1 - c)).wait_recv()

    def add(b, slot, n):
        @pl.loop(0, D // TV)
        def _(i):
            cols = pl.ds(pl.multiple_of(i * TV, 128), TV)
            total = own_b[b, :, cols] + sib_b[b, :, cols].astype(F32)
            for m in range(n):
                total = total + in_b[b, m, :, cols].astype(F32)
            if slot is None:
                own_b[b, :, cols] = total
            else:
                out_b[b, slot, :, cols] = total.astype(BF16)

    def sum_state(d, t):
        pos, nxt = step_of(d)
        first = jnp.where(pos == 0, SUMS - 1, SUMS + 6 * pos)
        on = (pos < 3) & (t >= first) & (t < SUMS + 20 - 2 * pos - jnp.where(pos == 0, 1, 0))
        u = jnp.clip(t - first, 0, 19)
        early = (pos == 0) & (u == NC)
        u = jnp.where((pos == 0) & (u > NC) & (u < 17), u - 1, u)
        k, j = jnp.where(early, 5, pos + 1 + u // NC), jnp.where(early, 0, u % NC)
        to_pos = jnp.where(k < 3, k + 1, 6 - k)
        idx = jnp.where(k < 3, y, 1 - y) * 4 + z_at(d, to_pos)
        return on, pos, nxt, k, j, idx

    def sum_send(d, t, nxt, k, j):
        return pltpu.make_async_remote_copy(
            out_b.at[d, t % 3], rows(ins.at[d], k * R + j * C, C), rs_send.at[d, t % 3],
            rs_recv.at[d, k * NC + j], **dev(y, nxt, c))

    def sum_loads(d, t):
        on, pos, _, k, j, idx = sum_state(d, t)

        @pl.when(on)
        def _():
            @pl.when(j == 0)
            def _():
                wait_partial(idx)

            own_load(d, idx, j).start()
            sib_load(d, idx, j).start()

            @pl.when(pos > 0)
            def _():
                wait_in(d, k, j)
                in_load(d, 0, d, k, j).start()

    def sum_drain(d, t):
        was, _, nxt, k, j, _ = sum_state(d, t - KEEP)

        @pl.when(was)
        def _():
            sum_send(d, t - KEEP, nxt, k, j).wait_send()

    def sum_add(d, t):
        sum_drain(d, t)
        on, pos, nxt, k, j, idx = sum_state(d, t)

        @pl.when(on)
        def _():
            own_load(d, idx, j).wait()
            sib_load(d, idx, j).wait()

            @pl.when(pos > 0)
            def _():
                in_load(d, 0, d, k, j).wait()
                add(d, t % 3, 1)

            @pl.when(pos == 0)
            def _():
                add(d, t % 3, 0)

            sum_send(d, t, nxt, k, j).start()

    end = 2

    def end_state(t):
        last = t >= OTHERS
        kind = jnp.where(last, 3, jnp.clip((t - PARTS) // NC, 0, 2))
        on = jnp.where(last, t < OTHERS + NC, (t >= PARTS) & (t < PARTS + 3 * NC))
        on = on & ((kind != 1) | (z < 3)) & ((kind != 2) | (z > 0))
        j = jnp.clip(jnp.where(last, t - OTHERS, (t - PARTS) % NC), 0, NC - 1)
        idx = jnp.where(kind == 3, 1 - y, y) * 4 + z + jnp.where(kind == 1, 1, 0) - jnp.where(kind == 2, 1, 0)
        idx = jnp.clip(idx, 0, 7)
        left = (z > 0) & ((kind == 1) | (kind == 3))
        right = (z < 3) & ((kind == 2) | (kind == 3))
        back = 3 - z
        arrived = (
            (0, left, jnp.where(kind == 1, z, 6 - z), 0),
            (1, right, jnp.where(kind == 2, back, 6 - back), jnp.where(left, 1, 0)),
        )
        return on, kind, j, idx, arrived

    def end_loads(t, start):
        on, _, j, idx, arrived = end_state(t)

        @pl.when(on)
        def _():
            if start:
                @pl.when(j == 0)
                def _():
                    wait_partial(idx)

            for copy in (own_load(end, idx, j), sib_load(end, idx, j)):
                copy.start() if start else copy.wait()
            for d, there, k, slot in arrived:
                @pl.when(there)
                def _(d=d, k=jnp.clip(k, 0, 5), slot=slot):
                    if start:
                        wait_in(d, k, j)
                        in_load(end, slot, d, k, j).start()
                    else:
                        in_load(end, slot, d, k, j).wait()

    def end_store(t, start):
        on, kind, j, _, _ = end_state(t)
        for n, (src, dst) in enumerate((
            (own_b.at[end], mysum), (out_b.at[end, 0], next_sum), (out_b.at[end, 0], back_sum), (out_b.at[end, 0], ysum),
        )):
            @pl.when(on & (kind == n))
            def _(src=src, dst=dst):
                copy = pltpu.make_async_copy(src, rows(dst, j * C, C), end_sem)
                copy.start() if start else copy.wait()

    def last_loads(t):
        end_store(t - 1, False)
        end_loads(t, True)

    def last_sum(t):
        end_loads(t, False)
        on, kind, _, _, ((_, left, _, _), (_, right, _, _)) = end_state(t)

        @pl.when(on & (kind == 0))
        def _():
            add(end, None, 0)

        for n, where in ((0, jnp.logical_not(left | right)), (1, left != right), (2, left & right)):
            @pl.when(on & (kind > 0) & where)
            def _(n=n):
                add(end, 0, n)

        end_store(t, True)

    def clear(ref):
        high = min(64, ref.shape[0])

        @pl.loop(0, ref.shape[0] // high)
        def _(i):
            ref[pl.ds(pl.multiple_of(i * high, 8), high), :] = jnp.zeros((high, ref.shape[1]), F32)

    def exchange(t, phase):
        def holds(first, last):
            return phase[0] <= last + KEEP and first < phase[1]

        arrivals = ((LAG, 11 + LAG, LAG, 15 + LAG), (NC + LAG, 23 + LAG, Y_X + LAG, Y_X3 + 9 + LATE))
        for a, (z_first, z_last, y_first, y_last) in enumerate(arrivals):
            if holds(z_first, z_last):
                for d in (0, 1):
                    arrive_z(d, a, t)
            if holds(y_first, y_last):
                arrive_y(a, t)
                if a:
                    arrive_y(a, t, True)
        for d in (0, 1):
            if holds(CUT + 3, CUT + 10):
                pass_cut(d, t, True)
        for a, (z_first, z_last, y_first, y_last) in enumerate(((0, 11, 0, 15), (NC, 23, Y_X, Y_X3 + 9))):
            if holds(y_first, y_last):
                gather_y(a, t)
                if a:
                    gather_y(a, t, True)
            if holds(z_first, z_last):
                for d in (0, 1):
                    gather_z(d, a, t)
        for d in (0, 1):
            if holds(CUT, CUT + 7):
                pass_cut(d, t, False)
        if holds(SUMS - 1, SUMS + 19):
            for d in (0, 1):
                sum_loads(d, t)
        last_loads(t)

    def sums(t):
        for d in (0, 1):
            sum_add(d, t)
        last_sum(t)

    def spread(t, begin, end, step):
        @pl.loop(0, jnp.maximum(end - begin, 2))
        def _(n):
            @pl.when(n == 1)
            def _():
                sums(t)

            @pl.when(begin + n < end)
            def _():
                step(begin + n)

    barrier = pltpu.get_barrier_semaphore()
    pl.semaphore_signal(barrier, 1, **dev(y, z, 1 - c))
    pl.semaphore_signal(barrier, 1, **dev(1 - y, z, c))

    @pl.when(z < 3)
    def _():
        pl.semaphore_signal(barrier, 1, **dev(y, z + 1, c))

    @pl.when(z > 0)
    def _():
        pl.semaphore_signal(barrier, 1, **dev(y, z - 1, c))

    pl.semaphore_wait(barrier, jnp.where((z > 0) & (z < 3), 4, 3))
    for a in (0, 1):
        own_to_sibling(a).start()

    def first(wd_v, wg_v, wu_v, dy_v, gate_v, up_v, dg_v, du_v, hid_v, stf, stb, w_sem, b_sem, dy_sem, g_sem, st_sem, dx_sem, dxs_send):
        weights = [pltpu.make_async_copy(h, v, w_sem.at[i]) for i, (h, v) in enumerate(((wd, wd_v), (wg, wg_v), (wu, wu_v)))]

        def block_of(n):
            other = (n == 2) | (n == 4) | (n >= 6)
            p = jnp.where(other, jnp.where(n == 7, 3, n // 2 - 1), jnp.where(n < 2, n, (n + 1) // 2))
            return jnp.where(other, 1 - y, y) * 4 + order(p, z)

        def gate_up(n):
            at = block_of(n) * B
            return [pltpu.make_async_copy(rows(h, at, B), v, g_sem.at[i]) for i, (h, v) in enumerate(((gate, gate_v), (up, up_v)))]

        def kept_grads(n):
            at = block_of(n) * B
            pairs = ((dg_v, dgs), (du_v, dus), (hid_v, hids))
            return [pltpu.make_async_copy(v, rows(h, at, B), st_sem.at[i]) for i, (v, h) in enumerate(pairs)]

        def own_rows(i, a):
            part = rows(dy_v, a * R, R)
            if i == 0:
                return pltpu.make_async_copy(sent[a], part, b_sem.at[a])
            return pltpu.make_async_copy(part, rows(kept[a], place(y, z, c), R), b_sem.at[a])

        def terms(n, tile, slot):
            at, cols = block_of(n) * R, pl.ds(pl.multiple_of(tile * TN, 128), TN)
            mine = pltpu.make_async_copy(
                stf.at[slot, pl.ds(pl.multiple_of(c * R, 8), R)], own.at[pl.ds(pl.multiple_of(at, 8), R), cols], dx_sem.at[slot])
            theirs = pltpu.make_async_remote_copy(
                stb.at[slot, pl.ds(pl.multiple_of((1 - c) * R, 8), R)], sib.at[pl.ds(pl.multiple_of(at, 8), R), cols],
                dxs_send.at[slot], dxs_recv.at[block_of(n)], **dev(y, z, 1 - c))
            return mine, theirs

        def wait_terms(n, tile, slot):
            mine, theirs = terms(n, tile, slot)
            mine.wait()
            theirs.wait_send()

        tiles = D // TN

        def drain(n):
            for copy in kept_grads(n):
                copy.wait()
            for tile in (tiles - 2, tiles - 1):
                wait_terms(n, tile, tile % 2)

        def gradients(n):
            @pl.when(n == 0)
            def _():
                weights[0].wait()

            for copy in gate_up(n):
                copy.wait()

            @pl.loop(0, F // TF)
            def _(i):
                cols = pl.ds(pl.multiple_of(i * TF, 128), TF)
                dh = lax.dot_general(
                    dy_v[...], wd_v[pl.ds(pl.multiple_of(i * TF, 128), TF), :], (((1,), (1,)), ((), ())), preferred_element_type=F32)
                g, u = gate_v[:, cols].astype(F32), up_v[:, cols].astype(F32)
                s = jax.nn.sigmoid(g)
                silu = g * s
                hid_v[:, cols] = (silu * u).astype(BF16)
                du_v[:, cols] = (dh * silu).astype(BF16)
                dg_v[:, cols] = ((dh * u) * (s * (1.0 + g * (1.0 - s)))).astype(BF16)

            for copy in kept_grads(n):
                copy.start()

            @pl.when(n < BLOCKS - 1)
            def _():
                for copy in gate_up(n + 1):
                    copy.start()

        def dx_terms(t, n):
            @pl.when(n == 0)
            def _():
                weights[1].wait()
                weights[2].wait()

            @pl.loop(0, tiles)
            def _(tile):
                @pl.when((tile == 1) & (t != SUMS - 1))
                def _():
                    sums(t)

                slot = tile % 2
                @pl.when(tile >= 2)
                def _():
                    wait_terms(n, tile - 2, slot)

                at = pl.ds(pl.multiple_of(tile * TN, 128), TN)
                nt = (((1,), (1,)), ((), ()))
                total = lax.dot_general(dg_v[...], wg_v[at, :], nt, preferred_element_type=F32)
                total = total + lax.dot_general(du_v[...], wu_v[at, :], nt, preferred_element_type=F32)
                stf[slot] = total
                stb[slot] = total.astype(BF16)
                mine, theirs = terms(n, tile, slot)
                mine.start()
                theirs.start()

            drain(n)

        @pl.loop(0, A_END)
        def _(t):
            @pl.when(t != SUMS - 1)
            def _():
                exchange(t, (0, A_END))

            @pl.when(t == 0)
            def _():
                for a in (0, 1):
                    own_rows(0, a).start()
                for copy in gate_up(0) + weights:
                    copy.start()

            @pl.when(t == 1)
            def _():
                for a in (0, 1):
                    own_rows(0, a).wait()
                    own_rows(1, a).start()
                for a in (0, 1):
                    own_rows(1, a).wait()

            n = jnp.clip((t - 3) // 2, 0, BLOCKS - 1)

            @pl.when((t == 2) | ((t >= 5) & (t % 2 == 1)))
            def _():
                idx = block_of(n)
                wait_sibling(0, idx)
                load = pltpu.make_async_copy(rows(gdy, idx * B, B), dy_v, dy_sem)
                load.start()

                sums(t)
                load.wait()
                gradients(n)

            @pl.when((t == 3) | ((t >= 6) & (t % 2 == 0)))
            def _():
                dx_terms(t, n)

                @pl.when(t == SUMS - 1)
                def _():
                    exchange(t, (0, A_END))
                    sums(t)

    pl.run_scoped(
        first,
        pltpu.VMEM((F, D), BF16), pltpu.VMEM((D, F), BF16), pltpu.VMEM((D, F), BF16),
        pltpu.VMEM((B, D), BF16), pltpu.VMEM((B, F), BF16), pltpu.VMEM((B, F), BF16),
        pltpu.VMEM((B, F), BF16), pltpu.VMEM((B, F), BF16), pltpu.VMEM((B, F), BF16),
        pltpu.VMEM((2, B, TN), F32), pltpu.VMEM((2, B, TN), BF16),
        pltpu.SemaphoreType.DMA((3,)), pltpu.SemaphoreType.DMA((2,)), pltpu.SemaphoreType.DMA,
        pltpu.SemaphoreType.DMA((2,)), pltpu.SemaphoreType.DMA((3,)), pltpu.SemaphoreType.DMA((2,)), pltpu.SemaphoreType.DMA((2,)),
    )

    def second(hid_v, dy_v, acc, out_v, h_sem, dy_sem, o_sem):
        depth, wide = T // TK, D // TND
        steps = depth * wide
        per_tick = -(-steps // (B_END - A_END))

        def tile(i):
            nt, kc = i // depth, i % depth
            return pltpu.make_async_copy(
                gdy.at[pl.ds(pl.multiple_of(kc * TK, 8), TK), pl.ds(pl.multiple_of(nt * TND, 128), TND)],
                dy_v.at[i % 2], dy_sem.at[i % 2])

        def result(nt):
            return pltpu.make_async_copy(out_v, dwd.at[:, pl.ds(pl.multiple_of(nt * TND, 128), TND)], o_sem)

        hidden = pltpu.make_async_copy(hids, hid_v, h_sem)
        hidden.start()
        tile(0).start()

        def step(i):
            nt, kc = i // depth, i % depth
            tile(i).wait()

            @pl.when(i + 1 < steps)
            def _():
                tile(i + 1).start()

            @pl.when(kc == 0)
            def _():
                clear(acc)

            acc[...] += lax.dot_general(
                hid_v[pl.ds(pl.multiple_of(kc * TK, 8), TK), :], dy_v[i % 2], (((0,), (0,)), ((), ())), preferred_element_type=F32)

            @pl.when(kc == depth - 1)
            def _():
                @pl.when(nt > 0)
                def _():
                    result(nt - 1).wait()

                out_v[...] = acc[...].astype(BF16)
                result(nt).start()

        @pl.loop(A_END, B_END)
        def _(t):
            exchange(t, (A_END, B_END))

            @pl.when(t == A_END)
            def _():
                hidden.wait()

            begin = (t - A_END) * per_tick
            spread(t, begin, jnp.minimum(begin + per_tick, steps), step)

        result(wide - 1).wait()

    pl.run_scoped(
        second,
        pltpu.VMEM((T, F), BF16), pltpu.VMEM((2, TK, TND), BF16), pltpu.VMEM((F, TND), F32), pltpu.VMEM((F, TND), BF16),
        pltpu.SemaphoreType.DMA, pltpu.SemaphoreType.DMA((2,)), pltpu.SemaphoreType.DMA,
    )

    def third(d_v, x_v, out_v, d_sem, x_sem, o_sem):
        steps = D // TM
        per_tick = -(-steps // (N_END - B_END))
        half = pl.ds(pl.multiple_of(y * 4 * B, 8), 4 * B)
        grads = [pltpu.make_async_copy(h.at[half], d_v.at[:, pl.ds(i * F, F)], d_sem.at[i]) for i, h in enumerate((dgs, dus))]

        def tile(i):
            return pltpu.make_async_copy(gx.at[half, pl.ds(pl.multiple_of(i * TM, 128), TM)], x_v.at[i % 2], x_sem.at[i % 2])

        def result(i):
            return pltpu.make_async_copy(out_v.at[i % 2], part.at[pl.ds(pl.multiple_of(i * TM, 8), TM)], o_sem.at[i % 2])

        def step(i):
            tile(i).wait()

            @pl.when(i + 1 < steps)
            def _():
                tile(i + 1).start()

            @pl.when(i >= 2)
            def _():
                result(i - 2).wait()

            out_v[i % 2] = lax.dot_general(x_v[i % 2], d_v[...], (((0,), (0,)), ((), ())), preferred_element_type=F32)
            result(i).start()

        for copy in grads:
            copy.start()

        @pl.loop(B_END, N_END)
        def _(t):
            exchange(t, (B_END, N_END))

            @pl.when(t == B_END)
            def _():
                for q in range(4):
                    wait_sibling(1, y * 4 + q)
                tile(0).start()
                for copy in grads:
                    copy.wait()

            begin = (t - B_END) * per_tick
            spread(t, begin, jnp.minimum(begin + per_tick, steps), step)

        for i in (steps - 2, steps - 1):
            result(i).wait()

    pl.run_scoped(
        third,
        pltpu.VMEM((4 * B, 2 * F), BF16), pltpu.VMEM((2, 4 * B, TM), BF16), pltpu.VMEM((2, TM, 2 * F), F32),
        pltpu.SemaphoreType.DMA((2,)), pltpu.SemaphoreType.DMA((2,)), pltpu.SemaphoreType.DMA((2,)),
    )

    @pl.loop(N_END, T_END)
    def _(t):
        exchange(t, (N_END, T_END))
        sums(t)

    for t in range(T_END, T_END + KEEP):
        arrive_y(1, t)
        arrive_y(1, t, True)
        for d in (0, 1):
            pass_cut(d, t, True)
    for q in range(4):
        wait_sibling(1, (1 - y) * 4 + q)
    for a in (0, 1):
        own_to_sibling(a).wait_send()


def finish_kernel(dims, part, gx, dgs, dus, down, dwg, dwu, dwd, d_v, x_v, p_v, out_v, down_v, d_sem, x_sem, p_sem, o_sem, c_sem):
    R, D, F, TM = dims[0], dims[1], dims[2], dims[5]
    steps, depth = D // TM, gx.shape[0] // 2
    half = pl.ds(pl.multiple_of((1 - lax.axis_index("tp") // 8) * depth, 8), depth)
    grads = [pltpu.make_async_copy(h.at[half], d_v.at[:, pl.ds(i * F, F)], d_sem.at[i]) for i, h in enumerate((dgs, dus))]
    pieces, high = 8, F // 8

    def tiles(i):
        at = pl.multiple_of(i * TM, 128)
        return [
            pltpu.make_async_copy(gx.at[half, pl.ds(at, TM)], x_v.at[i % 3], x_sem.at[i % 3]),
            pltpu.make_async_copy(part.at[pl.ds(at, TM)], p_v.at[i % 3], p_sem.at[i % 3]),
        ]

    def results(i):
        at = pl.ds(pl.multiple_of(i * TM, 8), TM)
        return [pltpu.make_async_copy(out_v.at[i % 2, n], h.at[at], o_sem.at[i % 2, n]) for n, h in enumerate((dwg, dwu))]

    def piece(way, i):
        at = pl.ds(pl.multiple_of(i * high, 8), high)
        if way == 0:
            return pltpu.make_async_copy(down.at[at], down_v.at[at], c_sem.at[0, i])
        return pltpu.make_async_copy(down_v.at[at], dwd.at[at], c_sem.at[1, i])

    for copy in grads + tiles(0) + tiles(1):
        copy.start()
    for copy in grads:
        copy.wait()

    @pl.loop(0, steps)
    def _(i):
        for copy in tiles(i):
            copy.wait()

        @pl.when(i + 2 < steps)
        def _():
            for copy in tiles(i + 2):
                copy.start()

        @pl.when(i < pieces)
        def _():
            piece(0, i).start()

        @pl.when((i >= 2) & (i < pieces + 2))
        def _():
            piece(0, i - 2).wait()
            piece(1, i - 2).start()

        @pl.when(i >= 2)
        def _():
            for copy in results(i - 2):
                copy.wait()

        total = p_v[i % 3] + lax.dot_general(x_v[i % 3], d_v[...], (((0,), (0,)), ((), ())), preferred_element_type=F32)
        for n in (0, 1):
            out_v[i % 2, n] = total[:, n * F : (n + 1) * F].astype(BF16)
        for copy in results(i):
            copy.start()

    for i in (steps - 2, steps - 1):
        for copy in results(i):
            copy.wait()
    for i in range(pieces):
        piece(1, i).wait()


def fused(dims, x, dy, gate, up, wg, wu, wd):
    R, D, F, TM = dims[0], dims[1], dims[2], dims[5]
    C, T = R // NC, 2 * R * BLOCKS
    hbm = pl.BlockSpec(memory_space=pl.ANY)
    shape, vmem, dma = jax.ShapeDtypeStruct, pltpu.VMEM, pltpu.SemaphoreType.DMA
    outs = (
        shape((R, D), BF16), shape((R, D), F32), shape((R, D), BF16), shape((R, D), BF16), shape((F, D), BF16), shape((D, 2 * F), F32),
        shape((T, D), BF16), shape((T, D), BF16), shape((T // 2, D), F32), shape((T // 2, D), BF16),
        shape((2, 6 * R, D), BF16), shape((T, F), BF16), shape((T, F), BF16), shape((T, F), BF16),
    )
    product = 2 * T * D * F
    ysum, mysum, next_sum, back_sum, down, part, gx, _, _, _, _, dgs, dus, _ = pl.pallas_call(
        functools.partial(kernel, dims),
        out_shape=outs,
        in_specs=[hbm] * 7,
        out_specs=[hbm] * len(outs),
        scratch_shapes=[
            vmem((3, C, D), F32), vmem((3, C, D), BF16), vmem((3, 2, C, D), BF16), vmem((3, 3, C, D), BF16),
            dma((2, 2, 4)), dma((2, 2, 12)), dma((2, 4)), dma((2, 16)), dma((2,)), dma((3, 2, 4)), dma((2, 8)), dma((2,)), dma((2,)),
            dma((2, 3)), dma((2, 3)), dma((2, 3)),
            dma((2, 3)), dma((2, 24)), dma((BLOCKS,)), dma((3, 4)), dma,
        ],
        compiler_params=pltpu.CompilerParams(collective_id=0, has_side_effects=True, vmem_limit_bytes=67043328),
        cost_estimate=pl.CostEstimate(flops=5 * product, bytes_accessed=10 * T * D, transcendentals=0),
        name="mlp_backward",
    )(x, dy, gate, up, wg, wu, wd)
    sums = [
        lax.ppermute(ysum, "tp", [(i, (i + 8) % 16) for i in range(16)]),
        lax.ppermute(next_sum, "tp", [(i, i + 2) for i in range(16) if i // 2 % 4 < 3]),
        lax.ppermute(back_sum, "tp", [(i, i - 2) for i in range(16) if i // 2 % 4 > 0]),
    ]
    weights = pl.pallas_call(
        functools.partial(finish_kernel, dims),
        out_shape=(shape((D, F), BF16), shape((D, F), BF16), shape((F, D), BF16)),
        in_specs=[hbm] * 5,
        out_specs=[hbm] * 3,
        scratch_shapes=[
            vmem((T // 2, 2 * F), BF16), vmem((3, T // 2, TM), BF16), vmem((3, TM, 2 * F), F32), vmem((2, 2, TM, F), BF16),
            vmem((F, D), BF16), dma((2,)), dma((3,)), dma((3,)), dma((2, 2)), dma((2, 8)),
        ],
        compiler_params=pltpu.CompilerParams(vmem_limit_bytes=67043328),
        cost_estimate=pl.CostEstimate(flops=product, bytes_accessed=6 * T * D, transcendentals=0),
        name="finish",
    )(part, gx, dgs, dus, down)
    return (sum((a.astype(F32) for a in sums), mysum).astype(BF16), *weights)


def solution(mesh):
    def step(x, dy, gate, up, wg, wu, wd):
        (rows, depth), wide = x.shape, wg.shape[1]
        dims = (rows, depth, wide, 512, 1024, 256, 1280, 512, 1024, 32)
        return fused(dims, x, dy, gate, up, wg, wu, wd)

    tokens, columns = P(("dp", "tp"), None), P("dp", "tp")
    return jax.shard_map(
        step,
        mesh=mesh,
        in_specs=(tokens, tokens, columns, columns, P(None, "tp"), P(None, "tp"), P("tp", None)),
        out_specs=(tokens, columns, columns, tokens),
        check_vma=False,
    )
```

```python
import functools

import jax
import jax.numpy as jnp
from jax import lax
from jax.experimental import pallas as pl
from jax.experimental.pallas import tpu as pltpu
from jax.sharding import PartitionSpec as P

MESH = pl.DeviceIdType.MESH
BF16, F32 = jnp.bfloat16, jnp.float32
NC = 4
BLOCKS = 8
LAG = 2
KEEP = 3
LATE = 3
Y_X, Y_X3 = 16, 20
CUT = 21
SUMS = 11
PARTS, OTHERS = 16, 28
A_END, B_END, N_END, T_END = 19, 25, 29, 33


BOTH, PAIR = (0, 1), 2
LAST = 3
LANES, ROWS = (((1,), (1,)), ((), ())), (((0,), (0,)), ((), ()))


def lanes(start, n):
    return pl.ds(pl.multiple_of(start, 128), n)


def subs(start, n):
    return pl.ds(pl.multiple_of(start, 8), n)


def order(p, z):
    near = jnp.where(z < 2, z, LAST - z)
    q = jnp.where((near == 1) & (p < 2), 1 - p, p)
    return jnp.where(z < 2, q, 3 - q)


def kernel(
    dims,
    x, dy, gate, up, wg, wu, wd,
    ysum, mysum, pair_sum, inner_sum, dwd, part, gx, gdy, own, sib, ins, dgs, dus, hids,
    own_b, sib_b, in_b, out_b,
    z_send, z_recv, y_send, y_recv, short_send, sib_send, sib_recv, sib_short, own_send, cut_send, cut_recv, cut_sib,
    rs_send, rs_recv, dxs_recv, load_sem, end_sem,
):
    R, D, F, TF, TN, TM, TND, TK, TV, CUT_ROWS = dims
    C, B, T = R // NC, 2 * R, 2 * R * BLOCKS
    dp, tp = lax.axis_index("dp"), lax.axis_index("tp")
    y, z, c = tp // 8, (tp // 2) % 4, tp % 2
    opp, mate = 1 - y, 1 - c
    sent, kept = (dy, x), (gdy, gx)

    def dev(yy, zz, cc):
        return dict(device_id=(dp, yy * 8 + zz * 2 + cc), device_id_type=MESH)

    def rows(ref, start, n):
        return ref.at[subs(start, n)]

    def place(yy, zz, cc):
        return ((yy * 4 + zz) * 2 + cc) * R

    def step_of(d):
        return (z, jnp.minimum(z + 1, LAST)) if d == 0 else (LAST - z, jnp.maximum(z - 1, 0))

    def z_at(d, pos):
        return pos if d == 0 else LAST - pos

    def gather_z(d, a, t):
        pos, nxt = step_of(d)
        base = a * NC * (pos + 1)

        def copy(t, own_rows=False):
            s = jnp.clip(t - base, 0, 11)
            p, j = s // NC, s % NC
            there = rows(kept[a], place(y, z_at(d, jnp.maximum(pos - p, 0)), c) + j * C, C)
            src = rows(sent[a], j * C, C) if own_rows else there
            return pltpu.make_async_remote_copy(
                src, there, z_send.at[d, a, t % 4], z_recv.at[d, a, s], **dev(y, nxt, c))

        def active(t):
            return (pos < LAST) & (t >= base) & (t < base + NC * (pos + 1))

        @pl.when(active(t - KEEP))
        def _():
            copy(t - KEEP).wait_send()

        @pl.when(active(t) & (t < base + NC))
        def _():
            copy(t, True).start()

        @pl.when(active(t) & (t >= base + NC))
        def _():
            copy(t).start()

    def to_sibling(a, ref_rows, idx, sem):
        return pltpu.make_async_remote_copy(ref_rows, ref_rows, sem, sib_recv.at[a, idx], **dev(y, z, mate))

    def arrive_z(d, a, t):
        pos, _ = step_of(d)
        base = a * NC * pos + LAG

        def chunk(t):
            r = jnp.clip(t - base, 0, 11)
            src_z = z_at(d, jnp.maximum(pos - 1 - r // NC, 0))
            return r, rows(kept[a], place(y, src_z, c) + (r % NC) * C, C), y * 4 + src_z

        def active(t):
            return (pos > 0) & (t >= base) & (t < base + NC * pos)

        @pl.when(active(t - KEEP))
        def _():
            _, ref, idx = chunk(t - KEEP)
            to_sibling(a, ref, idx, sib_send.at[d, a, (t - KEEP) % 4]).wait_send()

        @pl.when(active(t))
        def _():
            r, ref, idx = chunk(t)
            pltpu.make_async_remote_copy(
                ref, ref, z_send.at[d, a, 0], z_recv.at[d, a, r], **dev(y, z, mate)).wait_recv()
            to_sibling(a, ref, idx, sib_send.at[d, a, t % 4]).start()

    def y_chunk(a, t, short):
        if a == 0:
            s = jnp.clip(t, 0, 4 * NC - 1)
            return (t >= 0) & (t < 4 * NC), s // NC, s % NC, C
        v = jnp.clip(t - Y_X3, 0, 9)
        if short:
            return (t > Y_X3) & (t <= Y_X3 + 9) & (v % 3 == 0), jnp.maximum(v // 3, 1), 3, C - CUT_ROWS
        near = t < Y_X3
        return (t >= Y_X) & (t < Y_X3 + 9), jnp.where(near, 0, 1 + v // 3), jnp.where(near, jnp.clip(t - Y_X, 0, 3), v % 3), C

    def y_sems(a, t, short):
        return (short_send.at[(t // 3) % 2], sib_short.at[(t // 3) % 2]) if short else (y_send.at[a, t % 4], sib_send.at[2, a, t % 4])

    def gather_y(a, t, short=False):
        def copy(t, own_rows=False):
            _, p, j, high = y_chunk(a, t, short)
            there = rows(kept[a], place(y, order(p, z), c) + j * C, high)
            src = rows(sent[a], j * C, high) if own_rows else there
            return pltpu.make_async_remote_copy(src, there, y_sems(a, t, short)[0], y_recv.at[a, p * NC + j], **dev(opp, z, c))

        was, (on, p, _, _) = y_chunk(a, t - KEEP, short)[0], y_chunk(a, t, short)

        @pl.when(was)
        def _():
            copy(t - KEEP).wait_send()

        if not short:
            @pl.when(on & (p == 0))
            def _():
                copy(t, True).start()

        @pl.when(on & (p > 0))
        def _():
            copy(t).start()

    def arrive_y(a, t, short=False):
        def sent_at(t):
            if a == 0:
                return t - LAG
            return jnp.where(t < Y_X3 + LAG, t - LAG, jnp.where(t < Y_X3 + LATE, -1, t - LATE))

        def chunk(t):
            _, p, j, high = y_chunk(a, sent_at(t), short)
            q = order(p, z)
            return p * NC + j, rows(kept[a], place(opp, q, c) + j * C, high), opp * 4 + q

        @pl.when(y_chunk(a, sent_at(t - KEEP), short)[0])
        def _():
            _, ref, idx = chunk(t - KEEP)
            to_sibling(a, ref, idx, y_sems(a, t - KEEP, short)[1]).wait_send()

        @pl.when(y_chunk(a, sent_at(t), short)[0])
        def _():
            r, ref, idx = chunk(t)
            pltpu.make_async_remote_copy(ref, ref, y_send.at[a, 0], y_recv.at[a, r], **dev(opp, z, c)).wait_recv()
            to_sibling(a, ref, idx, y_sems(a, t, short)[1]).start()

    def pass_cut(d, t, arrive):
        pos, nxt = step_of(d)
        far = 1 if arrive else 0

        def state(t):
            ticks, last = ((CUT + 3, CUT + 6), (CUT + 6, CUT + 8, CUT + 10)) if arrive else ((CUT, CUT + 3), (CUT + 3, CUT + 4, CUT + 7))
            at_last = pos == 2 + far
            h = jnp.where(at_last, jnp.where(t == last[1], 1, jnp.where(t == last[2], 2, 0)), jnp.where(t == ticks[1], 1, 0))
            on = jnp.where(at_last, (t == last[0]) | (t == last[1]) | (t == last[2]), (t == ticks[0]) | (t == ticks[1]))
            on = on & (h + far <= pos) & (pos < LAST + far)
            q = z_at(d, jnp.maximum(pos - far - h, 0))
            ref = rows(gx, place(opp, q, c) + (R - CUT_ROWS), CUT_ROWS)
            if arrive:
                copy = to_sibling(1, ref, opp * 4 + q, cut_sib.at[d, h])
            else:
                copy = pltpu.make_async_remote_copy(ref, ref, cut_send.at[d, h], cut_recv.at[d, h], **dev(y, nxt, c))
            return on, h, ref, copy

        was, now = state(t - KEEP), state(t)

        @pl.when(was[0])
        def _():
            was[3].wait_send()

        @pl.when(now[0])
        def _():
            _, h, ref, copy = now
            if arrive:
                pltpu.make_async_remote_copy(ref, ref, cut_send.at[d, 0], cut_recv.at[d, h], **dev(y, z, mate)).wait_recv()
            copy.start()

    def own_to_sibling(a):
        return pltpu.make_async_remote_copy(
            sent[a], rows(kept[a], place(y, z, c), R), own_send.at[a], sib_recv.at[a, y * 4 + z], **dev(y, z, mate))

    def wait_sibling(a, idx):
        ref = rows(kept[a], idx * B, R)
        pltpu.make_async_remote_copy(ref, ref, own_send.at[a], sib_recv.at[a, idx], **dev(y, z, mate)).wait_recv()

    def wait_partial(idx):
        ref = rows(sib, idx * R, R)
        pltpu.make_async_remote_copy(ref, ref, own_send.at[0], dxs_recv.at[idx], **dev(y, z, mate)).wait_recv()

    def own_load(b, idx, j):
        return pltpu.make_async_copy(rows(own, idx * R + j * C, C), own_b.at[b], load_sem.at[b, 0])

    def sib_load(b, idx, j):
        return pltpu.make_async_copy(rows(sib, idx * R + j * C, C), sib_b.at[b], load_sem.at[b, 1])

    def in_load(b, n, d, k, j):
        return pltpu.make_async_copy(rows(ins.at[d], k * R + j * C, C), in_b.at[b, n], load_sem.at[b, 2 + n])

    def wait_in(d, k, j):
        ref = rows(ins.at[d], k * R + j * C, C)
        pltpu.make_async_remote_copy(
            ref, ref, rs_send.at[d, 0], rs_recv.at[d, k * NC + j], **dev(y, z, mate)).wait_recv()

    def add(b, slot, n):
        @pl.loop(0, D // TV)
        def _(i):
            cols = lanes(i * TV, TV)
            total = own_b[b, :, cols] + sib_b[b, :, cols].astype(F32)
            for m in range(n):
                total = total + in_b[b, m, :, cols].astype(F32)
            if slot is None:
                own_b[b, :, cols] = total
            else:
                out_b[b, slot, :, cols] = total.astype(BF16)

    def sum_state(d, t):
        pos, nxt = step_of(d)
        first = jnp.where(pos == 0, SUMS - 1, SUMS + 6 * pos)
        on = (pos < LAST) & (t >= first) & (t < SUMS + 20 - 2 * pos - jnp.where(pos == 0, 1, 0))
        u = jnp.clip(t - first, 0, 19)
        early = (pos == 0) & (u == NC)
        u = jnp.where((pos == 0) & (u > NC) & (u < 17), u - 1, u)
        k, j = jnp.where(early, 5, pos + 1 + u // NC), jnp.where(early, 0, u % NC)
        to_pos = jnp.where(k < 3, k + 1, 6 - k)
        idx = jnp.where(k < 3, y, opp) * 4 + z_at(d, to_pos)
        return on, pos, nxt, k, j, idx

    def sum_send(d, t, nxt, k, j):
        return pltpu.make_async_remote_copy(
            out_b.at[d, t % 3], rows(ins.at[d], k * R + j * C, C), rs_send.at[d, t % 3],
            rs_recv.at[d, k * NC + j], **dev(y, nxt, c))

    def sum_loads(d, t):
        on, pos, _, k, j, idx = sum_state(d, t)

        @pl.when(on)
        def _():
            @pl.when(j == 0)
            def _():
                wait_partial(idx)

            own_load(d, idx, j).start()
            sib_load(d, idx, j).start()

            @pl.when(pos > 0)
            def _():
                wait_in(d, k, j)
                in_load(d, 0, d, k, j).start()

    def sum_drain(d, t):
        was, _, nxt, k, j, _ = sum_state(d, t - KEEP)

        @pl.when(was)
        def _():
            sum_send(d, t - KEEP, nxt, k, j).wait_send()

    def sum_add(d, t):
        sum_drain(d, t)
        on, pos, nxt, k, j, idx = sum_state(d, t)

        @pl.when(on)
        def _():
            own_load(d, idx, j).wait()
            sib_load(d, idx, j).wait()

            @pl.when(pos > 0)
            def _():
                in_load(d, 0, d, k, j).wait()
                add(d, t % 3, 1)

            @pl.when(pos == 0)
            def _():
                add(d, t % 3, 0)

            sum_send(d, t, nxt, k, j).start()

    end = 2

    def end_state(t):
        last = t >= OTHERS
        kind = jnp.where(last, 3, jnp.clip((t - PARTS) // NC, 0, 2))
        on = jnp.where(last, t < OTHERS + NC, (t >= PARTS) & (t < PARTS + 3 * NC))
        on = on & ((kind != 1) | (z < LAST)) & ((kind != 2) | (z > 0))
        j = jnp.clip(jnp.where(last, t - OTHERS, (t - PARTS) % NC), 0, NC - 1)
        idx = jnp.where(kind == 3, opp, y) * 4 + z + jnp.where(kind == 1, 1, 0) - jnp.where(kind == 2, 1, 0)
        idx = jnp.clip(idx, 0, 7)
        left = (z > 0) & ((kind == 1) | (kind == 3))
        right = (z < LAST) & ((kind == 2) | (kind == 3))
        back = LAST - z
        arrived = (
            (0, left, jnp.where(kind == 1, z, 6 - z), 0),
            (1, right, jnp.where(kind == 2, back, 6 - back), jnp.where(left, 1, 0)),
        )
        return on, kind, j, idx, arrived

    def end_loads(t, start):
        on, _, j, idx, arrived = end_state(t)

        @pl.when(on)
        def _():
            if start:
                @pl.when(j == 0)
                def _():
                    wait_partial(idx)

            for copy in (own_load(end, idx, j), sib_load(end, idx, j)):
                copy.start() if start else copy.wait()
            for d, there, k, slot in arrived:
                @pl.when(there)
                def _(d=d, k=jnp.clip(k, 0, 5), slot=slot):
                    if start:
                        wait_in(d, k, j)
                        in_load(end, slot, d, k, j).start()
                    else:
                        in_load(end, slot, d, k, j).wait()

    def end_store(t, start):
        on, kind, j, _, _ = end_state(t)
        along = (kind == 1) | (kind == 2)
        paired = (kind == 1) == (z % 2 == 0)
        for where, src, dst in (
            (kind == 0, own_b.at[end], mysum),
            (along & paired, out_b.at[end, 0], pair_sum),
            (along & jnp.logical_not(paired), out_b.at[end, 0], inner_sum),
            (kind == 3, out_b.at[end, 0], ysum),
        ):
            @pl.when(on & where)
            def _(src=src, dst=dst):
                copy = pltpu.make_async_copy(src, rows(dst, j * C, C), end_sem)
                copy.start() if start else copy.wait()

    def last_loads(t):
        end_store(t - 1, False)
        end_loads(t, True)

    def last_sum(t):
        end_loads(t, False)
        on, kind, _, _, ((_, left, _, _), (_, right, _, _)) = end_state(t)

        @pl.when(on & (kind == 0))
        def _():
            add(end, None, 0)

        for n, where in ((0, jnp.logical_not(left | right)), (1, left != right), (2, left & right)):
            @pl.when(on & (kind > 0) & where)
            def _(n=n):
                add(end, 0, n)

        end_store(t, True)

    def clear(ref):
        high = min(64, ref.shape[0])

        @pl.loop(0, ref.shape[0] // high)
        def _(i):
            ref[subs(i * high, high), :] = jnp.zeros((high, ref.shape[1]), F32)

    def exchange(t, phase):
        def holds(first, last):
            return phase[0] <= last + KEEP and first < phase[1]

        arrivals = ((LAG, 11 + LAG, LAG, 15 + LAG), (NC + LAG, 23 + LAG, Y_X + LAG, Y_X3 + 9 + LATE))
        for a, (z_first, z_last, y_first, y_last) in enumerate(arrivals):
            if holds(z_first, z_last):
                for d in BOTH:
                    arrive_z(d, a, t)
            if holds(y_first, y_last):
                arrive_y(a, t)
                if a:
                    arrive_y(a, t, True)
        for d in BOTH:
            if holds(CUT + 3, CUT + 10):
                pass_cut(d, t, True)
        for a, (z_first, z_last, y_first, y_last) in enumerate(((0, 11, 0, 15), (NC, 23, Y_X, Y_X3 + 9))):
            if holds(y_first, y_last):
                gather_y(a, t)
                if a:
                    gather_y(a, t, True)
            if holds(z_first, z_last):
                for d in BOTH:
                    gather_z(d, a, t)
        for d in BOTH:
            if holds(CUT, CUT + 7):
                pass_cut(d, t, False)
        if holds(SUMS - 1, SUMS + 19):
            for d in BOTH:
                sum_loads(d, t)
        last_loads(t)

    def sums(t):
        for d in BOTH:
            sum_add(d, t)
        last_sum(t)

    def spread(t, begin, end, step):
        @pl.loop(0, jnp.maximum(end - begin, 2))
        def _(n):
            @pl.when(n == 1)
            def _():
                sums(t)

            @pl.when(begin + n < end)
            def _():
                step(begin + n)

    barrier = pltpu.get_barrier_semaphore()
    pl.semaphore_signal(barrier, 1, **dev(y, z, mate))
    pl.semaphore_signal(barrier, 1, **dev(opp, z, c))

    @pl.when(z < LAST)
    def _():
        pl.semaphore_signal(barrier, 1, **dev(y, z + 1, c))

    @pl.when(z > 0)
    def _():
        pl.semaphore_signal(barrier, 1, **dev(y, z - 1, c))

    pl.semaphore_wait(barrier, jnp.where((z > 0) & (z < LAST), 4, 3))
    for a in BOTH:
        own_to_sibling(a).start()

    def first(wd_v, wg_v, wu_v, dy_v, gate_v, up_v, dg_v, du_v, hid_v, stf, stb, w_sem, b_sem, dy_sem, g_sem, st_sem, dx_sem, dxs_send):
        weights = [pltpu.make_async_copy(h, v, w_sem.at[i]) for i, (h, v) in enumerate(((wd, wd_v), (wg, wg_v), (wu, wu_v)))]

        def block_of(n):
            other = (n == 2) | (n == 4) | (n >= 6)
            p = jnp.where(other, jnp.where(n == 7, 3, n // 2 - 1), jnp.where(n < 2, n, (n + 1) // 2))
            return jnp.where(other, opp, y) * 4 + order(p, z)

        def gate_up(n):
            at = block_of(n) * B
            return [pltpu.make_async_copy(rows(h, at, B), v, g_sem.at[i]) for i, (h, v) in enumerate(((gate, gate_v), (up, up_v)))]

        def kept_grads(n):
            at = block_of(n) * B
            pairs = ((dg_v, dgs), (du_v, dus), (hid_v, hids))
            return [pltpu.make_async_copy(v, rows(h, at, B), st_sem.at[i]) for i, (v, h) in enumerate(pairs)]

        def own_rows(i, a):
            part = rows(dy_v, a * R, R)
            if i == 0:
                return pltpu.make_async_copy(sent[a], part, b_sem.at[a])
            return pltpu.make_async_copy(part, rows(kept[a], place(y, z, c), R), b_sem.at[a])

        def terms(n, tile, slot):
            at, cols = block_of(n) * R, lanes(tile * TN, TN)
            mine = pltpu.make_async_copy(
                stf.at[slot, subs(c * R, R)], own.at[subs(at, R), cols], dx_sem.at[slot])
            theirs = pltpu.make_async_remote_copy(
                stb.at[slot, subs(mate * R, R)], sib.at[subs(at, R), cols],
                dxs_send.at[slot], dxs_recv.at[block_of(n)], **dev(y, z, mate))
            return mine, theirs

        def wait_terms(n, tile, slot):
            mine, theirs = terms(n, tile, slot)
            mine.wait()
            theirs.wait_send()

        tiles = D // TN

        def drain(n):
            for copy in kept_grads(n):
                copy.wait()
            for tile in (tiles - 2, tiles - 1):
                wait_terms(n, tile, tile % PAIR)

        def gradients(n):
            @pl.when(n == 0)
            def _():
                weights[0].wait()

            for copy in gate_up(n):
                copy.wait()

            @pl.loop(0, F // TF)
            def _(i):
                cols = lanes(i * TF, TF)
                dh = lax.dot_general(
                    dy_v[...], wd_v[lanes(i * TF, TF), :], LANES, preferred_element_type=F32)
                g, u = gate_v[:, cols].astype(F32), up_v[:, cols].astype(F32)
                s = jax.nn.sigmoid(g)
                silu = g * s
                hid_v[:, cols] = (silu * u).astype(BF16)
                du_v[:, cols] = (dh * silu).astype(BF16)
                dg_v[:, cols] = ((dh * u) * (s * (1.0 + g * (1.0 - s)))).astype(BF16)

            for copy in kept_grads(n):
                copy.start()

            @pl.when(n < BLOCKS - 1)
            def _():
                for copy in gate_up(n + 1):
                    copy.start()

        def dx_terms(t, n):
            @pl.when(n == 0)
            def _():
                weights[1].wait()
                weights[2].wait()

            @pl.loop(0, tiles)
            def _(tile):
                @pl.when((tile == 1) & (t != SUMS - 1))
                def _():
                    sums(t)

                slot = tile % PAIR
                @pl.when(tile >= 2)
                def _():
                    wait_terms(n, tile - 2, slot)

                at = lanes(tile * TN, TN)
                nt = LANES
                total = lax.dot_general(dg_v[...], wg_v[at, :], nt, preferred_element_type=F32)
                total = total + lax.dot_general(du_v[...], wu_v[at, :], nt, preferred_element_type=F32)
                stf[slot] = total
                stb[slot] = total.astype(BF16)
                mine, theirs = terms(n, tile, slot)
                mine.start()
                theirs.start()

            drain(n)

        @pl.loop(0, A_END)
        def _(t):
            @pl.when(t != SUMS - 1)
            def _():
                exchange(t, (0, A_END))

            @pl.when(t == 0)
            def _():
                for a in BOTH:
                    own_rows(0, a).start()
                for copy in gate_up(0) + weights:
                    copy.start()

            @pl.when(t == 1)
            def _():
                for a in BOTH:
                    own_rows(0, a).wait()
                    own_rows(1, a).start()
                for a in BOTH:
                    own_rows(1, a).wait()

            n = jnp.clip((t - 3) // 2, 0, BLOCKS - 1)

            @pl.when((t == 2) | ((t >= 5) & (t % 2 == 1)))
            def _():
                idx = block_of(n)
                wait_sibling(0, idx)
                load = pltpu.make_async_copy(rows(gdy, idx * B, B), dy_v, dy_sem)
                load.start()

                sums(t)
                load.wait()
                gradients(n)

            @pl.when((t == 3) | ((t >= 6) & (t % 2 == 0)))
            def _():
                dx_terms(t, n)

                @pl.when(t == SUMS - 1)
                def _():
                    exchange(t, (0, A_END))
                    sums(t)

    pl.run_scoped(
        first,
        pltpu.VMEM((F, D), BF16), pltpu.VMEM((D, F), BF16), pltpu.VMEM((D, F), BF16),
        pltpu.VMEM((B, D), BF16), pltpu.VMEM((B, F), BF16), pltpu.VMEM((B, F), BF16),
        pltpu.VMEM((B, F), BF16), pltpu.VMEM((B, F), BF16), pltpu.VMEM((B, F), BF16),
        pltpu.VMEM((PAIR, B, TN), F32), pltpu.VMEM((PAIR, B, TN), BF16),
        pltpu.SemaphoreType.DMA((3,)), pltpu.SemaphoreType.DMA((PAIR,)), pltpu.SemaphoreType.DMA,
        pltpu.SemaphoreType.DMA((PAIR,)), pltpu.SemaphoreType.DMA((3,)), pltpu.SemaphoreType.DMA((PAIR,)), pltpu.SemaphoreType.DMA((PAIR,)),
    )

    def second(hid_v, dy_v, acc, out_v, h_sem, dy_sem, o_sem):
        depth, wide = T // TK, D // TND
        steps = depth * wide
        per_tick = -(-steps // (B_END - A_END))

        def tile(i):
            nt, kc = i // depth, i % depth
            return pltpu.make_async_copy(
                gdy.at[subs(kc * TK, TK), lanes(nt * TND, TND)],
                dy_v.at[i % PAIR], dy_sem.at[i % PAIR])

        def result(nt):
            return pltpu.make_async_copy(out_v, dwd.at[:, lanes(nt * TND, TND)], o_sem)

        hidden = pltpu.make_async_copy(hids, hid_v, h_sem)
        hidden.start()
        tile(0).start()

        def step(i):
            nt, kc = i // depth, i % depth
            tile(i).wait()

            @pl.when(i + 1 < steps)
            def _():
                tile(i + 1).start()

            @pl.when(kc == 0)
            def _():
                clear(acc)

            acc[...] += lax.dot_general(
                hid_v[subs(kc * TK, TK), :], dy_v[i % PAIR], ROWS, preferred_element_type=F32)

            @pl.when(kc == depth - 1)
            def _():
                @pl.when(nt > 0)
                def _():
                    result(nt - 1).wait()

                out_v[...] = acc[...].astype(BF16)
                result(nt).start()

        @pl.loop(A_END, B_END)
        def _(t):
            exchange(t, (A_END, B_END))

            @pl.when(t == A_END)
            def _():
                hidden.wait()

            begin = (t - A_END) * per_tick
            spread(t, begin, jnp.minimum(begin + per_tick, steps), step)

        result(wide - 1).wait()

    pl.run_scoped(
        second,
        pltpu.VMEM((T, F), BF16), pltpu.VMEM((PAIR, TK, TND), BF16), pltpu.VMEM((F, TND), F32), pltpu.VMEM((F, TND), BF16),
        pltpu.SemaphoreType.DMA, pltpu.SemaphoreType.DMA((PAIR,)), pltpu.SemaphoreType.DMA,
    )

    def third(d_v, x_v, out_v, d_sem, x_sem, o_sem):
        steps = D // TM
        per_tick = -(-steps // (N_END - B_END))
        half = subs(y * 4 * B, 4 * B)
        grads = [pltpu.make_async_copy(h.at[half], d_v.at[:, pl.ds(i * F, F)], d_sem.at[i]) for i, h in enumerate((dgs, dus))]

        def tile(i):
            return pltpu.make_async_copy(gx.at[half, lanes(i * TM, TM)], x_v.at[i % PAIR], x_sem.at[i % PAIR])

        def result(i):
            return pltpu.make_async_copy(out_v.at[i % PAIR], part.at[subs(i * TM, TM)], o_sem.at[i % PAIR])

        def step(i):
            tile(i).wait()

            @pl.when(i + 1 < steps)
            def _():
                tile(i + 1).start()

            @pl.when(i >= 2)
            def _():
                result(i - 2).wait()

            out_v[i % PAIR] = lax.dot_general(x_v[i % PAIR], d_v[...], ROWS, preferred_element_type=F32)
            result(i).start()

        for copy in grads:
            copy.start()

        @pl.loop(B_END, N_END)
        def _(t):
            exchange(t, (B_END, N_END))

            @pl.when(t == B_END)
            def _():
                for q in range(4):
                    wait_sibling(1, y * 4 + q)
                tile(0).start()
                for copy in grads:
                    copy.wait()

            begin = (t - B_END) * per_tick
            spread(t, begin, jnp.minimum(begin + per_tick, steps), step)

        for i in (steps - 2, steps - 1):
            result(i).wait()

    pl.run_scoped(
        third,
        pltpu.VMEM((4 * B, 2 * F), BF16), pltpu.VMEM((PAIR, 4 * B, TM), BF16), pltpu.VMEM((PAIR, TM, 2 * F), F32),
        pltpu.SemaphoreType.DMA((PAIR,)), pltpu.SemaphoreType.DMA((PAIR,)), pltpu.SemaphoreType.DMA((PAIR,)),
    )

    @pl.loop(N_END, T_END)
    def _(t):
        exchange(t, (N_END, T_END))
        sums(t)

    for t in range(T_END, T_END + KEEP):
        arrive_y(1, t)
        arrive_y(1, t, True)
        for d in BOTH:
            pass_cut(d, t, True)
    for q in range(4):
        wait_sibling(1, opp * 4 + q)
    for a in BOTH:
        own_to_sibling(a).wait_send()


def finish_kernel(dims, part, gx, dgs, dus, down, dwg, dwu, dwd, d_v, x_v, p_v, out_v, down_v, d_sem, x_sem, p_sem, o_sem, c_sem):
    R, D, F, TM = dims[0], dims[1], dims[2], dims[5]
    steps, depth = D // TM, gx.shape[0] // 2
    half = subs((1 - lax.axis_index("tp") // 8) * depth, depth)
    grads = [pltpu.make_async_copy(h.at[half], d_v.at[:, pl.ds(i * F, F)], d_sem.at[i]) for i, h in enumerate((dgs, dus))]
    pieces, high = 8, F // 8

    def tiles(i):
        at = pl.multiple_of(i * TM, 128)
        return [
            pltpu.make_async_copy(gx.at[half, pl.ds(at, TM)], x_v.at[i % 3], x_sem.at[i % 3]),
            pltpu.make_async_copy(part.at[pl.ds(at, TM)], p_v.at[i % 3], p_sem.at[i % 3]),
        ]

    def results(i):
        at = subs(i * TM, TM)
        return [pltpu.make_async_copy(out_v.at[i % PAIR, n], h.at[at], o_sem.at[i % PAIR, n]) for n, h in enumerate((dwg, dwu))]

    def piece(way, i):
        at = subs(i * high, high)
        if way == 0:
            return pltpu.make_async_copy(down.at[at], down_v.at[at], c_sem.at[0, i])
        return pltpu.make_async_copy(down_v.at[at], dwd.at[at], c_sem.at[1, i])

    for copy in grads + tiles(0) + tiles(1):
        copy.start()
    for copy in grads:
        copy.wait()

    @pl.loop(0, steps)
    def _(i):
        for copy in tiles(i):
            copy.wait()

        @pl.when(i + 2 < steps)
        def _():
            for copy in tiles(i + 2):
                copy.start()

        @pl.when(i < pieces)
        def _():
            piece(0, i).start()

        @pl.when((i >= 2) & (i < pieces + 2))
        def _():
            piece(0, i - 2).wait()
            piece(1, i - 2).start()

        @pl.when(i >= 2)
        def _():
            for copy in results(i - 2):
                copy.wait()

        total = p_v[i % 3] + lax.dot_general(x_v[i % 3], d_v[...], ROWS, preferred_element_type=F32)
        for n in BOTH:
            out_v[i % PAIR, n] = total[:, n * F : (n + 1) * F].astype(BF16)
        for copy in results(i):
            copy.start()

    for i in (steps - 2, steps - 1):
        for copy in results(i):
            copy.wait()
    for i in range(pieces):
        piece(1, i).wait()


def fused(dims, x, dy, gate, up, wg, wu, wd):
    R, D, F, TM = dims[0], dims[1], dims[2], dims[5]
    C, T = R // NC, 2 * R * BLOCKS
    hbm = pl.BlockSpec(memory_space=pl.ANY)
    shape, vmem, dma = jax.ShapeDtypeStruct, pltpu.VMEM, pltpu.SemaphoreType.DMA
    outs = (
        shape((R, D), BF16), shape((R, D), F32), shape((R, D), BF16), shape((R, D), BF16), shape((F, D), BF16), shape((D, 2 * F), F32),
        shape((T, D), BF16), shape((T, D), BF16), shape((T // 2, D), F32), shape((T // 2, D), BF16),
        shape((2, 6 * R, D), BF16), shape((T, F), BF16), shape((T, F), BF16), shape((T, F), BF16),
    )
    product = 2 * T * D * F
    ysum, mysum, pair_sum, inner_sum, down, part, gx, _, _, _, _, dgs, dus, _ = pl.pallas_call(
        functools.partial(kernel, dims),
        out_shape=outs,
        in_specs=[hbm] * 7,
        out_specs=[hbm] * len(outs),
        scratch_shapes=[
            vmem((3, C, D), F32), vmem((3, C, D), BF16), vmem((3, 2, C, D), BF16), vmem((3, 3, C, D), BF16),
            dma((PAIR, PAIR, 4)), dma((PAIR, PAIR, 12)), dma((PAIR, 4)), dma((PAIR, 16)), dma((PAIR,)), dma((3, 2, 4)), dma((PAIR, 8)), dma((PAIR,)), dma((PAIR,)),
            dma((PAIR, 3)), dma((PAIR, 3)), dma((PAIR, 3)),
            dma((PAIR, 3)), dma((PAIR, 24)), dma((BLOCKS,)), dma((3, 4)), dma,
        ],
        compiler_params=pltpu.CompilerParams(collective_id=0, has_side_effects=True, vmem_limit_bytes=67043328),
        cost_estimate=pl.CostEstimate(flops=5 * product, bytes_accessed=10 * T * D, transcendentals=0),
        name="mlp_backward",
    )(x, dy, gate, up, wg, wu, wd)
    around, spots = range(16), [i // 2 % 4 for i in range(16)]
    sums = [
        lax.ppermute(ysum, "tp", [(i, (i + 8) % 16) for i in around]),
        lax.ppermute(pair_sum, "tp", [(i, i ^ 2) for i in around]),
        lax.ppermute(inner_sum, "tp", [(i, i + 2 if spots[i] == 1 else i - 2) for i in around if 0 < spots[i] < 3]),
    ]
    weights = pl.pallas_call(
        functools.partial(finish_kernel, dims),
        out_shape=(shape((D, F), BF16), shape((D, F), BF16), shape((F, D), BF16)),
        in_specs=[hbm] * 5,
        out_specs=[hbm] * 3,
        scratch_shapes=[
            vmem((T // 2, 2 * F), BF16), vmem((3, T // 2, TM), BF16), vmem((3, TM, 2 * F), F32), vmem((PAIR, 2, TM, F), BF16),
            vmem((F, D), BF16), dma((PAIR,)), dma((3,)), dma((3,)), dma((PAIR, 2)), dma((PAIR, 8)),
        ],
        compiler_params=pltpu.CompilerParams(vmem_limit_bytes=67043328),
        cost_estimate=pl.CostEstimate(flops=product, bytes_accessed=6 * T * D, transcendentals=0),
        name="finish",
    )(part, gx, dgs, dus, down)
    return (sum((a.astype(F32) for a in sums), mysum).astype(BF16), *weights)


def solution(mesh):
    def step(x, dy, gate, up, wg, wu, wd):
        (rows, depth), wide = x.shape, wg.shape[1]
        dims = (rows, depth, wide, 512, 1024, 256, 1280, 512, 1024, 32)
        return fused(dims, x, dy, gate, up, wg, wu, wd)

    tokens, columns = P(("dp", "tp"), None), P("dp", "tp")
    return jax.shard_map(
        step,
        mesh=mesh,
        in_specs=(tokens, tokens, columns, columns, P(None, "tp"), P(None, "tp"), P("tp", None)),
        out_specs=(tokens, columns, columns, tokens),
        check_vma=False,
    )
```
